32 devices in a mesh: row: 8 (over z, core), col: 4 (over y, x).
Axes of the slice: x: 2, y: 2, z: 4, core: 2. Of those that a mesh axis runs over, the one named last changes fastest.
Arguments:
- substrate: float32 [1024, 1024], P('row', 'col'), may hold values from 0.05 to 0.95
- activator: float32 [1024, 1024], P('row', 'col'), may hold values from 0 to 0.45
Outputs:
- substrate_section: float32 [1024, 1024], P('row', 'col')
- activator_section: float32 [1024, 1024], P('row', 'col')
The draws below stay inside these ranges and needn't reach their ends.
All inputs are finite; a program needn't handle non-finite values.
Results may differ from the reference program's by a relative error of at most 0.00023.
Values sent between devices are 32-bit elements; how exact they have to be, the bound alone decides.
No kernel may reach another device: no remote copies, remote signals or barrier semaphores. Data moves between devices by JAX's collectives and lax.ppermute only.
A program may use at most 64 MiB of HBM per device.

```python
import math
import jax
import jax.numpy as jnp

NX = 1024
NY = 1024


def smooth_part(key):
    orders = jnp.arange(1, 5, dtype=jnp.float32)
    row_coords = jnp.arange(NX, dtype=jnp.float32) / NX
    col_coords = jnp.arange(NY, dtype=jnp.float32) / NY
    row_angles = 2.0 * math.pi * orders[:, None] * row_coords[None, :]
    col_angles = 2.0 * math.pi * orders[:, None] * col_coords[None, :]
    basis_rows = jnp.concatenate([jnp.cos(row_angles), jnp.sin(row_angles)], axis=0)
    basis_cols = jnp.concatenate([jnp.cos(col_angles), jnp.sin(col_angles)], axis=0)
    coefficients = jax.random.normal(key, (8, 8), jnp.float32)
    mixed = jnp.dot(coefficients, basis_cols, preferred_element_type=jnp.float32)
    return jnp.dot(basis_rows.T, mixed, preferred_element_type=jnp.float32) / 4.0


def draw_substrate(key, part):
    smooth = smooth_part(jax.random.fold_in(key, 11))
    rough_key = jax.random.fold_in(key, 12)
    rough_part = jax.random.uniform(rough_key, (NX, NY), jnp.float32, -1.0, 1.0)
    return (0.55 + 0.2 * jnp.tanh(smooth) + 0.15 * rough_part).astype(jnp.float32)


def draw_activator(key, part):
    smooth = smooth_part(jax.random.fold_in(key, 23))
    rough_key = jax.random.fold_in(key, 24)
    rough_part = jax.random.uniform(rough_key, (NX, NY), jnp.float32, -1.0, 1.0)
    return (0.25 + 0.08 * jnp.tanh(smooth) + 0.08 * rough_part).astype(jnp.float32)


def setup_inputs(seed: int = 0) -> dict:
    key_of = jax.random.split(jax.random.key(seed), 3)
    substrate = draw_substrate(jax.random.fold_in(key_of[2], 71), 0)
    activator = draw_activator(jax.random.fold_in(key_of[2], 71), 0)
    return dict(substrate=substrate, activator=activator)


FEED_RATE = 0.037
KILL_RATE = 0.06
TIME_STEP = 8.0
SUBSTRATE_DIFFUSION = 4e-7
ACTIVATOR_DIFFUSION = 2e-7


def signed_squares(total):
    indices = jnp.arange(total, dtype=jnp.int32)
    signed = jnp.where(2 * indices < total, indices, indices - total).astype(jnp.float32)
    angular = (2.0 * math.pi) * signed
    return angular * angular


def section_factors(wave_number, diffusion, decay_rate):
    linear = -diffusion * wave_number - decay_rate
    exponent = linear * (0.5 * TIME_STEP)
    return jnp.exp(exponent), jnp.expm1(exponent) / linear


def species_section(field, source, wave_number, diffusion, decay_rate):
    growth, forcing = section_factors(wave_number, diffusion, decay_rate)
    spectrum = jnp.fft.fft2(field + 1j * source)
    advanced = spectrum * (growth - 1j * forcing)
    return jnp.real(jnp.fft.ifft2(advanced)).astype(jnp.float32)


def reference(substrate, activator):
    reaction = substrate * activator * activator
    wave_number = signed_squares(NX)[:, None] + signed_squares(NY)[None, :]
    substrate_section = species_section(substrate, FEED_RATE - reaction, wave_number, SUBSTRATE_DIFFUSION, FEED_RATE)
    activator_section = species_section(activator, reaction, wave_number, ACTIVATOR_DIFFUSION, FEED_RATE + KILL_RATE)
    return (substrate_section, activator_section)
```

```python
import math

import jax
import jax.numpy as jnp
import numpy as np
from jax import lax
from jax.experimental import pallas as pl
from jax.experimental.pallas import tpu as pltpu
from jax.sharding import PartitionSpec as P

FEED_RATE = 0.037
KILL_RATE = 0.06
TIME_STEP = 8.0
SUBSTRATE_DIFFUSION = 4e-07
ACTIVATOR_DIFFUSION = 2e-07
LANES = 128
SUBLANES = 8
VMEM = pl.BlockSpec(memory_space=pltpu.VMEM)
SMEM = pl.BlockSpec(memory_space=pltpu.SMEM)


def basis_matrices(total):
    radix = total // LANES
    b = np.arange(LANES, dtype=np.int64)[:, None]
    k2 = np.arange(LANES, dtype=np.int64)[None, :]

    def angles(k1):
        return (b * (k1 + radix * k2) % total) * (2.0 * np.pi / total)

    matrices = np.zeros((radix // 2, 2 * LANES, 2 * LANES))
    for half, k1 in enumerate((0, radix // 2)):
        theta = angles(k1)
        part = slice(half * LANES, (half + 1) * LANES)
        matrices[0, part, part] = np.cos(theta) + np.sin(theta)
    for k1 in range(1, radix // 2):
        cosine, sine = np.cos(angles(k1)), np.sin(angles(k1))
        matrices[k1] = np.block([[cosine, -sine], [sine, cosine]])
    return matrices


def split_constant(matrices):
    high = matrices.astype(jnp.bfloat16)
    low = (matrices - high.astype(np.float64)).astype(jnp.bfloat16)
    return jnp.asarray(high), jnp.asarray(low)


def split_value(values):
    high = values.astype(jnp.bfloat16)
    low = (values - high.astype(jnp.float32)).astype(jnp.bfloat16)
    return high, low


def dot(left, right):
    return jnp.dot(left, right, preferred_element_type=jnp.float32)


def dot_pairs(left, right):
    return dot(left[0], right[0]) + (dot(left[0], right[1]) + dot(left[1], right[0]))


def turn(value, k, period, sign):
    real, imag = value
    if k == 0:
        return value
    if 4 * k == period:
        return (-sign * imag, sign * real) if imag is not None else (None, sign * real)
    cosine, sine = math.cos(2.0 * math.pi * k / period), sign * math.sin(2.0 * math.pi * k / period)
    if imag is None:
        return (real * cosine, real * sine)
    if 8 * k == period:
        return ((real - sign * imag) * cosine, (imag + sign * real) * cosine)
    return (real * cosine - imag * sine, real * sine + imag * cosine)


def plus(left, right):
    if left is None or right is None:
        return left if right is None else right
    return left + right


def minus(left, right):
    if right is None:
        return left
    return -right if left is None else left - right


def real_dft(values):
    n = len(values)
    if n == 1:
        return [(values[0], None)]
    even, odd = real_dft(values[0::2]), real_dft(values[1::2])
    out = [None] * (n // 2 + 1)
    for k in range(n // 4 + 1):
        turned = turn(odd[k], k, n, -1.0)
        if n // 2 - k != k:
            out[n // 2 - k] = (minus(even[k][0], turned[0]), minus(turned[1], even[k][1]))
        out[k] = (plus(even[k][0], turned[0]), plus(even[k][1], turned[1]))
    return out


def real_dft_transposed(spectrum):
    n = 2 * (len(spectrum) - 1)
    if n == 0:
        return [spectrum[0][0]]
    even, odd = [], []
    for k in range(n // 4 + 1):
        near, far = spectrum[k], spectrum[n // 2 - k]
        if k == 0:
            even.append((near[0] + far[0], None))
            odd.append((near[0] - far[0], None))
        elif 4 * k == n:
            even.append((near[0], None))
            odd.append((-near[1], None))
        else:
            even.append((near[0] + far[0], near[1] - far[1]))
            odd.append(turn((near[0] - far[0], near[1] + far[1]), k, n, 1.0))
    out = [None] * n
    out[0::2] = real_dft_transposed(even)
    out[1::2] = real_dft_transposed(odd)
    return out


def paired(spectrum, axis):
    half = len(spectrum) - 1
    rows = [(spectrum[0][0], spectrum[half][0])] + spectrum[1:half]
    return [jnp.concatenate(row, axis=axis) for row in rows]


def unpaired(products, axis):
    def halves(value):
        return lax.slice_in_dim(value, 0, LANES, axis=axis), lax.slice_in_dim(value, LANES, 2 * LANES, axis=axis)

    parts = [halves(value) for value in products]
    first, last = parts[0]
    return [(first, None)] + parts[1:] + [(last, None)]


def lane_chunk(shape, width):
    return lax.broadcasted_iota(jnp.int32, shape, len(shape) - 1) // width


def pick_chunks(pieces, width):
    chunk = lane_chunk(pieces[0].shape, width)
    out = pieces[-1]
    for index in range(len(pieces) - 2, -1, -1):
        out = jnp.where(chunk == index, pieces[index], out)
    return out


def rolled(value, chunks, width):
    shift = chunks * width % LANES
    return pltpu.roll(value, shift, 1) if shift else value


def wave_squares(k1, k2, total):
    radix = total // LANES
    wave = k1 + radix * k2
    signed = jnp.where(2 * wave < total, wave, wave - total).astype(jnp.float32)
    angular = (2.0 * math.pi) * signed
    return angular * angular


def tables_kernel(total_rows, total_cols, width, device_ref, growth_ref, forcing_ref):
    radix = total_rows // LANES
    chunks = LANES // width
    device = device_ref[0]
    tile, place = device // chunks, device % chunks
    lane = lax.broadcasted_iota(jnp.int32, (1, LANES), 1)
    col_class = jnp.where(tile == 0, 0, jnp.where(tile == 1, total_cols // LANES // 2, tile // 2))
    col_squares = wave_squares(col_class, place * width + lane % width, total_cols)
    col_scale = jnp.where(tile < 2, 1.0 / total_cols, 2.0 / total_cols).astype(jnp.float32)
    first = lane < width
    diffusion = jnp.where(first, SUBSTRATE_DIFFUSION, ACTIVATOR_DIFFUSION).astype(jnp.float32)
    decay = jnp.where(first, FEED_RATE, FEED_RATE + KILL_RATE).astype(jnp.float32)
    sign = jnp.where(first, -1.0, 1.0).astype(jnp.float32)
    k2 = lax.broadcasted_iota(jnp.int32, (LANES, LANES), 0)
    for index in range(radix // 2):
        for half in range(2):
            k1 = half * (radix // 2) if index == 0 else index
            scale = col_scale * ((1.0 if index == 0 else 2.0) / total_rows)
            linear = -diffusion * (wave_squares(k1, k2, total_rows) + col_squares) - decay
            growth = jnp.exp(linear * (0.5 * TIME_STEP))
            rows = slice(half * LANES, (half + 1) * LANES)
            growth_ref[index, rows, :] = growth * scale
            forcing_ref[index, rows, :] = (growth - 1.0) / linear * (scale * sign)


def forward_kernel(packed, place_ref, *refs):
    *block_refs, high_ref, low_ref, out_ref, buffer_ref = refs
    count = len(block_refs)
    place = place_ref[0]
    for step, block_ref in enumerate(block_refs):
        buffer_ref[place ^ step] = block_ref[...]
    cols = buffer_ref.shape[-1]
    height = buffer_ref.shape[2]
    tiles = []
    for source in range(count):
        for tile in range(cols // LANES):
            part = slice(tile * LANES, (tile + 1) * LANES)
            substrate = buffer_ref[source, 0, :, part]
            activator = buffer_ref[source, 1, :, part]
            tiles.append(jnp.concatenate([substrate, activator, substrate * activator * activator], axis=0))
    operands = paired(real_dft(tiles), 1)
    for index, operand in enumerate(operands):
        product = dot_pairs(split_value(operand), (high_ref[index], low_ref[index]))
        for half in range(2):
            tile = 2 * index + half
            spectrum = product[:, half * LANES : (half + 1) * LANES]
            if not packed:
                out_ref[tile] = spectrum
                continue
            width = LANES // count
            turns = [rolled(spectrum, shift, width) for shift in range(count)]
            for chunk in range(count):
                for field in range(3):
                    base = field * height
                    pieces = [
                        turns[(group - chunk) % count][base + group * SUBLANES : base + (group + 1) * SUBLANES]
                        for group in range(count)
                    ]
                    out_ref[tile * count + chunk, field * SUBLANES : (field + 1) * SUBLANES, :] = pick_chunks(
                        pieces, width
                    )


def advance_kernel(packed, count, *refs):
    if packed:
        in_ref, growth_ref, forcing_ref, high_ref, low_ref, high_t_ref, low_t_ref, out_ref = refs
        width = LANES // count
        radix = in_ref.shape[0] // count
        tiles = []
        for band in range(radix):
            own_rows, source_rows = [], []
            for source in range(count):
                block = in_ref[band * count + source]
                turns = [
                    [rolled(block[field * SUBLANES : (field + 1) * SUBLANES], -shift, width) for shift in range(count)]
                    for field in range(3)
                ]
                low_half = lane_chunk((SUBLANES, LANES), width) == 0
                for group in range(count):
                    near, next_near = group, (group - 1) % count
                    own_rows.append(jnp.where(low_half, turns[0][near], turns[1][next_near]))
                    source_rows.append(jnp.where(low_half, turns[2][near], turns[2][next_near]))
            own = jnp.concatenate(own_rows, axis=0)
            tiles.append(jnp.concatenate([own, jnp.concatenate(source_rows, axis=0)], axis=1))
    else:
        own_ref, source_ref, growth_ref, forcing_ref, high_ref, low_ref, high_t_ref, low_t_ref, out_ref = refs
        radix = own_ref.shape[0]
        tiles = [jnp.concatenate([own_ref[band], source_ref[band]], axis=1) for band in range(radix)]
    operands = paired(real_dft(tiles), 0)
    products = []
    for index, operand in enumerate(operands):
        spectrum = dot_pairs((high_t_ref[index], low_t_ref[index]), split_value(operand))
        advanced = growth_ref[index] * spectrum[:, :LANES] + forcing_ref[index] * spectrum[:, LANES:]
        products.append(dot_pairs((high_ref[index], low_ref[index]), split_value(advanced)))
    bands = real_dft_transposed(unpaired(products, 0))
    for band, value in enumerate(bands):
        if not packed:
            out_ref[band] = value
            continue
        height = LANES // count
        for target in range(count):
            for field in range(2):
                pieces = [
                    rolled(
                        value[target * height + group * SUBLANES : target * height + (group + 1) * SUBLANES],
                        group - field,
                        width,
                    )
                    for group in range(count)
                ]
                out_ref[band * count + target, field * SUBLANES : (field + 1) * SUBLANES, :] = pick_chunks(
                    pieces, width
                )


def inverse_kernel(packed, count, shift, place_ref, in_ref, high_t_ref, low_t_ref, out_ref):
    place = place_ref[0]
    radix = 2 * high_t_ref.shape[0]
    height = out_ref.shape[2]
    cols = out_ref.shape[3]
    tiles = []
    for tile in range(radix):
        if not packed:
            tiles.append(in_ref[tile])
            continue
        width = LANES // count
        turns = [[rolled(in_ref[tile * count + chunk], step, width) for step in range(count)] for chunk in range(count)]
        rows = []
        for field in range(2):
            part = slice(field * SUBLANES, (field + 1) * SUBLANES)
            for group in range(count):
                rows.append(
                    pick_chunks([turns[chunk][(chunk - group) % count][part] for chunk in range(count)], width)
                )
        tiles.append(jnp.concatenate(rows, axis=0))
    products = []
    for index in range(radix // 2):
        operand = jnp.concatenate([tiles[2 * index], tiles[2 * index + 1]], axis=1)
        products.append(dot_pairs(split_value(operand), (high_t_ref[index], low_t_ref[index])))
    values = real_dft_transposed(unpaired(products, 1))
    per_target = cols // LANES
    for index, value in enumerate(values):
        target, tile = index // per_target, index % per_target
        part = slice(tile * LANES, (tile + 1) * LANES)
        out_ref[place ^ target, 0, :, part] = value[:height] + shift
        out_ref[place ^ target, 1, :, part] = value[height:]


def call(kernel, out_shape, specs, operands, scratch=()):
    return pl.pallas_call(
        kernel,
        out_shape=out_shape,
        in_specs=specs,
        out_specs=jax.tree.map(lambda _: VMEM, out_shape),
        scratch_shapes=list(scratch),
    )(*operands)


def float_shape(*shape):
    return jax.ShapeDtypeStruct(shape, jnp.float32)


def swap_blocks(blocks):
    count = len(blocks)
    return [blocks[0]] + [
        lax.ppermute(blocks[step], "col", [(s, s ^ step) for s in range(count)]) for step in range(1, count)
    ]


def on_device(substrate, activator):
    row_count, col_count = substrate.shape
    bands, count = lax.axis_size("row"), lax.axis_size("col")
    total_rows, total_cols = row_count * bands, col_count * count
    height = row_count // count
    radix = total_cols // LANES
    width = total_cols // (bands * count)
    assert row_count == LANES and total_rows == total_cols and count & (count - 1) == 0
    packed = height == SUBLANES * count and width * count == LANES
    place = lax.axis_index("col")
    places = place[None].astype(jnp.int32)
    devices = (lax.axis_index("row") * count + place)[None].astype(jnp.int32)
    matrices = basis_matrices(total_rows)
    high, low = split_constant(matrices)
    high_t, low_t = split_constant(np.swapaxes(matrices, 1, 2))

    fields = jnp.stack([substrate, activator]).reshape(2, count, height, col_count)
    blocks = swap_blocks(
        [lax.dynamic_index_in_dim(fields, place ^ step, 1, keepdims=False) for step in range(count)]
    )
    growth, forcing = call(
        lambda *refs: tables_kernel(total_rows, total_cols, width, *refs),
        [float_shape(radix // 2, 2 * LANES, LANES)] * 2,
        [SMEM],
        (devices,),
    )
    spectra = call(
        lambda *refs: forward_kernel(packed, *refs),
        float_shape(bands * count, 3 * SUBLANES, LANES) if packed else float_shape(radix, 3 * height, LANES),
        [SMEM] + [VMEM] * (count + 2),
        (places, *blocks, high, low),
        [pltpu.VMEM((count, 2, height, col_count), jnp.float32)],
    )
    axes = ("row", "col")
    if packed:
        spectra = (lax.all_to_all(spectra, axes, 0, 0, tiled=True),)
    else:
        spectra = spectra.reshape(radix, 3, height, LANES // width, width)
        spectra = jnp.transpose(spectra, (0, 3, 1, 2, 4)).reshape(bands * count, -1)
        spectra = lax.all_to_all(spectra, axes, 0, 0, tiled=True)
        spectra = jnp.transpose(spectra.reshape(bands, count, 3, height, width), (2, 0, 1, 3, 4))
        spectra = spectra.reshape(3, bands, row_count, width)
        rest = jnp.zeros((bands, row_count, LANES - 2 * width), jnp.float32)
        spectra = (
            jnp.concatenate([spectra[0], spectra[1], rest], axis=2),
            jnp.concatenate([spectra[2], spectra[2], rest], axis=2),
        )
    advanced = call(
        lambda *refs: advance_kernel(packed, count, *refs),
        float_shape(bands * count, 2 * SUBLANES, LANES) if packed else float_shape(bands, row_count, LANES),
        [VMEM] * (len(spectra) + 6),
        (*spectra, growth, forcing, high, low, high_t, low_t),
    )
    if packed:
        advanced = lax.all_to_all(advanced, axes, 0, 0, tiled=True)
    else:
        advanced = advanced[:, :, : 2 * width].reshape(bands, count, height, 2, width)
        advanced = jnp.transpose(advanced, (0, 1, 3, 2, 4)).reshape(bands * count, -1)
        advanced = lax.all_to_all(advanced, axes, 0, 0, tiled=True)
        advanced = jnp.transpose(advanced.reshape(radix, LANES // width, 2, height, width), (0, 2, 3, 1, 4))
        advanced = advanced.reshape(radix, 2 * height, LANES)
    shift = FEED_RATE * math.expm1(-FEED_RATE * 0.5 * TIME_STEP) / -FEED_RATE
    values = call(
        lambda *refs: inverse_kernel(packed, count, shift, *refs),
        float_shape(count, 2, height, col_count),
        [SMEM] + [VMEM] * 3,
        (places, advanced, high_t, low_t),
    )
    blocks = swap_blocks([values[step] for step in range(count)])
    out = jnp.zeros((2, count, height, col_count), jnp.float32)
    for step, block in enumerate(blocks):
        out = lax.dynamic_update_index_in_dim(out, block, place ^ step, 1)
    out = out.reshape(2, row_count, col_count)
    return (out[0], out[1])


def solution(mesh):
    in_specs = (P("row", "col"), P("row", "col"))
    out_specs = (P("row", "col"), P("row", "col"))
    return jax.shard_map(
        on_device, mesh=mesh, in_specs=in_specs, out_specs=out_specs, check_vma=False
    )
```

```python
import math

import jax
import jax.numpy as jnp
import numpy as np
from jax import lax
from jax.experimental import pallas as pl
from jax.experimental.pallas import tpu as pltpu
from jax.sharding import PartitionSpec as P

FEED_RATE = 0.037
KILL_RATE = 0.06
TIME_STEP = 8.0
SUBSTRATE_DIFFUSION = 4e-07
ACTIVATOR_DIFFUSION = 2e-07
LANES = 128
SUBLANES = 8
VMEM_LIMIT = 36 << 20
VMEM = pl.BlockSpec(memory_space=pltpu.VMEM)
SMEM = pl.BlockSpec(memory_space=pltpu.SMEM)


def basis_matrices(total):
    radix = total // LANES
    b = np.arange(LANES, dtype=np.int64)[:, None]
    k2 = np.arange(LANES, dtype=np.int64)[None, :]

    def angles(k1):
        return (b * (k1 + radix * k2) % total) * (2.0 * np.pi / total)

    matrices = np.zeros((radix // 2, 2 * LANES, 2 * LANES))
    for half, k1 in enumerate((0, radix // 2)):
        theta = angles(k1)
        part = slice(half * LANES, (half + 1) * LANES)
        matrices[0, part, part] = np.cos(theta) + np.sin(theta)
    for k1 in range(1, radix // 2):
        cosine, sine = np.cos(angles(k1)), np.sin(angles(k1))
        matrices[k1] = np.block([[cosine, -sine], [sine, cosine]])
    return matrices


def split_constant(matrices):
    high = matrices.astype(jnp.bfloat16)
    low = (matrices - high.astype(np.float64)).astype(jnp.bfloat16)
    return jnp.asarray(high), jnp.asarray(low)


def split_value(values):
    high = values.astype(jnp.bfloat16)
    low = (values - high.astype(jnp.float32)).astype(jnp.bfloat16)
    return high, low


def dot(left, right):
    return jnp.dot(left, right, preferred_element_type=jnp.float32)


def dot_pairs(left, right):
    return dot(left[0], right[0]) + (dot(left[0], right[1]) + dot(left[1], right[0]))


def turn(value, k, period, sign):
    real, imag = value
    if k == 0:
        return value
    if 4 * k == period:
        return (-sign * imag, sign * real) if imag is not None else (None, sign * real)
    cosine, sine = math.cos(2.0 * math.pi * k / period), sign * math.sin(2.0 * math.pi * k / period)
    if imag is None:
        return (real * cosine, real * sine)
    if 8 * k == period:
        return ((real - sign * imag) * cosine, (imag + sign * real) * cosine)
    return (real * cosine - imag * sine, real * sine + imag * cosine)


def plus(left, right):
    if left is None or right is None:
        return left if right is None else right
    return left + right


def minus(left, right):
    if right is None:
        return left
    return -right if left is None else left - right


def real_dft(values):
    n = len(values)
    if n == 1:
        return [(values[0], None)]
    even, odd = real_dft(values[0::2]), real_dft(values[1::2])
    out = [None] * (n // 2 + 1)
    for k in range(n // 4 + 1):
        turned = turn(odd[k], k, n, -1.0)
        if n // 2 - k != k:
            out[n // 2 - k] = (minus(even[k][0], turned[0]), minus(turned[1], even[k][1]))
        out[k] = (plus(even[k][0], turned[0]), plus(even[k][1], turned[1]))
    return out


def real_dft_transposed(spectrum):
    n = 2 * (len(spectrum) - 1)
    if n == 0:
        return [spectrum[0][0]]
    even, odd = [], []
    for k in range(n // 4 + 1):
        near, far = spectrum[k], spectrum[n // 2 - k]
        if k == 0:
            even.append((near[0] + far[0], None))
            odd.append((near[0] - far[0], None))
        elif 4 * k == n:
            even.append((near[0], None))
            odd.append((-near[1], None))
        else:
            even.append((near[0] + far[0], near[1] - far[1]))
            odd.append(turn((near[0] - far[0], near[1] + far[1]), k, n, 1.0))
    out = [None] * n
    out[0::2] = real_dft_transposed(even)
    out[1::2] = real_dft_transposed(odd)
    return out


def paired(spectrum, axis):
    half = len(spectrum) - 1
    rows = [(spectrum[0][0], spectrum[half][0])] + spectrum[1:half]
    return [jnp.concatenate(row, axis=axis) for row in rows]


def unpaired(products, axis):
    def halves(value):
        return lax.slice_in_dim(value, 0, LANES, axis=axis), lax.slice_in_dim(value, LANES, 2 * LANES, axis=axis)

    parts = [halves(value) for value in products]
    first, last = parts[0]
    return [(first, None)] + parts[1:] + [(last, None)]


def lane_chunk(shape, width):
    return lax.broadcasted_iota(jnp.int32, shape, len(shape) - 1) // width


def pick_chunks(pieces, width):
    chunk = lane_chunk(pieces[0].shape, width)
    out = pieces[-1]
    for index in range(len(pieces) - 2, -1, -1):
        out = jnp.where(chunk == index, pieces[index], out)
    return out


def rolled(value, chunks, width):
    shift = chunks * width % LANES
    return pltpu.roll(value, shift, 1) if shift else value


def wave_squares(k1, k2, total):
    radix = total // LANES
    wave = k1 + radix * k2
    signed = jnp.where(2 * wave < total, wave, wave - total).astype(jnp.float32)
    angular = (2.0 * math.pi) * signed
    return angular * angular


def tables_kernel(total_rows, total_cols, width, device_ref, growth_ref, forcing_ref):
    radix = total_rows // LANES
    chunks = LANES // width
    device = device_ref[0]
    tile, place = device // chunks, device % chunks
    lane = lax.broadcasted_iota(jnp.int32, (1, LANES), 1)
    col_class = jnp.where(tile == 0, 0, jnp.where(tile == 1, total_cols // LANES // 2, tile // 2))
    col_squares = wave_squares(col_class, place * width + lane % width, total_cols)
    col_scale = jnp.where(tile < 2, 1.0 / total_cols, 2.0 / total_cols).astype(jnp.float32)
    first = lane < width
    diffusion = jnp.where(first, SUBSTRATE_DIFFUSION, ACTIVATOR_DIFFUSION).astype(jnp.float32)
    decay = jnp.where(first, FEED_RATE, FEED_RATE + KILL_RATE).astype(jnp.float32)
    sign = jnp.where(first, -1.0, 1.0).astype(jnp.float32)
    k2 = lax.broadcasted_iota(jnp.int32, (LANES, LANES), 0)
    for index in range(radix // 2):
        for half in range(2):
            k1 = half * (radix // 2) if index == 0 else index
            scale = col_scale * ((1.0 if index == 0 else 2.0) / total_rows)
            linear = -diffusion * (wave_squares(k1, k2, total_rows) + col_squares) - decay
            growth = jnp.exp(linear * (0.5 * TIME_STEP))
            rows = slice(half * LANES, (half + 1) * LANES)
            growth_ref[index, rows, :] = growth * scale
            forcing_ref[index, rows, :] = (growth - 1.0) / linear * (scale * sign)


def forward_kernel(packed, place_ref, *refs):
    *block_refs, high_ref, low_ref, _, out_ref, buffer_ref = refs
    count = len(block_refs)
    place = place_ref[0]
    for step, block_ref in enumerate(block_refs):
        buffer_ref[place ^ step] = block_ref[...]
    cols = buffer_ref.shape[-1]
    height = buffer_ref.shape[2]
    tiles = []
    for source in range(count):
        for tile in range(cols // LANES):
            part = slice(tile * LANES, (tile + 1) * LANES)
            substrate = buffer_ref[source, 0, :, part]
            activator = buffer_ref[source, 1, :, part]
            tiles.append(jnp.concatenate([substrate, activator, substrate * activator * activator], axis=0))
    operands = paired(real_dft(tiles), 1)
    for index, operand in enumerate(operands):
        product = dot_pairs(split_value(operand), (high_ref[index], low_ref[index]))
        for half in range(2):
            tile = 2 * index + half
            spectrum = product[:, half * LANES : (half + 1) * LANES]
            if not packed:
                out_ref[tile] = spectrum
                continue
            width = LANES // count
            turns = [rolled(spectrum, shift, width) for shift in range(count)]
            for chunk in range(count):
                for field in range(3):
                    base = field * height
                    pieces = [
                        turns[(group - chunk) % count][base + group * SUBLANES : base + (group + 1) * SUBLANES]
                        for group in range(count)
                    ]
                    out_ref[tile * count + chunk, field * SUBLANES : (field + 1) * SUBLANES, :] = pick_chunks(
                        pieces, width
                    )


def advance_kernel(packed, count, *refs):
    if packed:
        in_ref, growth_ref, forcing_ref, high_ref, low_ref, high_t_ref, low_t_ref, out_ref = refs
        width = LANES // count
        radix = in_ref.shape[0] // count
        tiles = []
        for band in range(radix):
            own_rows, source_rows = [], []
            for source in range(count):
                block = in_ref[band * count + source]
                turns = [
                    [rolled(block[field * SUBLANES : (field + 1) * SUBLANES], -shift, width) for shift in range(count)]
                    for field in range(3)
                ]
                low_half = lane_chunk((SUBLANES, LANES), width) == 0
                for group in range(count):
                    near, next_near = group, (group - 1) % count
                    own_rows.append(jnp.where(low_half, turns[0][near], turns[1][next_near]))
                    source_rows.append(jnp.where(low_half, turns[2][near], turns[2][next_near]))
            own = jnp.concatenate(own_rows, axis=0)
            tiles.append(jnp.concatenate([own, jnp.concatenate(source_rows, axis=0)], axis=1))
    else:
        own_ref, source_ref, growth_ref, forcing_ref, high_ref, low_ref, high_t_ref, low_t_ref, out_ref = refs
        radix = own_ref.shape[0]
        tiles = [jnp.concatenate([own_ref[band], source_ref[band]], axis=1) for band in range(radix)]
    operands = paired(real_dft(tiles), 0)
    products = []
    for index, operand in enumerate(operands):
        spectrum = dot_pairs((high_t_ref[index], low_t_ref[index]), split_value(operand))
        advanced = growth_ref[index] * spectrum[:, :LANES] + forcing_ref[index] * spectrum[:, LANES:]
        products.append(dot_pairs((high_ref[index], low_ref[index]), split_value(advanced)))
    bands = real_dft_transposed(unpaired(products, 0))
    for band, value in enumerate(bands):
        if not packed:
            out_ref[band] = value
            continue
        height = LANES // count
        for target in range(count):
            for field in range(2):
                pieces = [
                    rolled(
                        value[target * height + group * SUBLANES : target * height + (group + 1) * SUBLANES],
                        group - field,
                        width,
                    )
                    for group in range(count)
                ]
                out_ref[band * count + target, field * SUBLANES : (field + 1) * SUBLANES, :] = pick_chunks(
                    pieces, width
                )


def inverse_kernel(packed, count, shift, place_ref, in_ref, high_t_ref, low_t_ref, out_ref):
    place = place_ref[0]
    radix = 2 * high_t_ref.shape[0]
    height = out_ref.shape[2]
    cols = out_ref.shape[3]
    tiles = []
    for tile in range(radix):
        if not packed:
            tiles.append(in_ref[tile])
            continue
        width = LANES // count
        turns = [[rolled(in_ref[tile * count + chunk], step, width) for step in range(count)] for chunk in range(count)]
        rows = []
        for field in range(2):
            part = slice(field * SUBLANES, (field + 1) * SUBLANES)
            for group in range(count):
                rows.append(
                    pick_chunks([turns[chunk][(chunk - group) % count][part] for chunk in range(count)], width)
                )
        tiles.append(jnp.concatenate(rows, axis=0))
    products = []
    for index in range(radix // 2):
        operand = jnp.concatenate([tiles[2 * index], tiles[2 * index + 1]], axis=1)
        products.append(dot_pairs(split_value(operand), (high_t_ref[index], low_t_ref[index])))
    values = real_dft_transposed(unpaired(products, 1))
    per_target = cols // LANES
    for index, value in enumerate(values):
        target, tile = index // per_target, index % per_target
        part = slice(tile * LANES, (tile + 1) * LANES)
        out_ref[place ^ target, 0, :, part] = value[:height] + shift
        out_ref[place ^ target, 1, :, part] = value[height:]


def call(kernel, out_shape, specs, operands, scratch=()):
    return pl.pallas_call(
        kernel,
        out_shape=out_shape,
        in_specs=specs,
        out_specs=jax.tree.map(lambda _: VMEM, out_shape),
        scratch_shapes=list(scratch),
        compiler_params=pltpu.CompilerParams(vmem_limit_bytes=VMEM_LIMIT),
    )(*operands)


def float_shape(*shape):
    return jax.ShapeDtypeStruct(shape, jnp.float32)


def swap_blocks(blocks):
    count = len(blocks)
    return [blocks[0]] + [
        lax.ppermute(blocks[step], "col", [(s, s ^ step) for s in range(count)]) for step in range(1, count)
    ]


def on_device(substrate, activator):
    row_count, col_count = substrate.shape
    bands, count = lax.axis_size("row"), lax.axis_size("col")
    total_rows, total_cols = row_count * bands, col_count * count
    height = row_count // count
    radix = total_cols // LANES
    width = total_cols // (bands * count)
    assert row_count == LANES and total_rows == total_cols and count & (count - 1) == 0
    packed = height == SUBLANES * count and width * count == LANES
    place = lax.axis_index("col")
    places = place[None].astype(jnp.int32)
    devices = (lax.axis_index("row") * count + place)[None].astype(jnp.int32)
    matrices = basis_matrices(total_rows)
    high, low = split_constant(matrices)
    high_t, low_t = split_constant(np.swapaxes(matrices, 1, 2))

    fields = jnp.stack([substrate, activator]).reshape(2, count, height, col_count)
    blocks = swap_blocks(
        [lax.dynamic_index_in_dim(fields, place ^ step, 1, keepdims=False) for step in range(count)]
    )
    growth, forcing = call(
        lambda *refs: tables_kernel(total_rows, total_cols, width, *refs),
        [float_shape(radix // 2, 2 * LANES, LANES)] * 2,
        [SMEM],
        (devices,),
    )
    spectra = call(
        lambda *refs: forward_kernel(packed, *refs),
        float_shape(bands * count, 3 * SUBLANES, LANES) if packed else float_shape(radix, 3 * height, LANES),
        [SMEM] + [VMEM] * (count + 2) + [pl.BlockSpec(memory_space=pl.ANY)],
        (places, *blocks, high, low, growth),
        [pltpu.VMEM((count, 2, height, col_count), jnp.float32)],
    )
    axes = ("row", "col")
    if packed:
        spectra = (lax.all_to_all(spectra, axes, 0, 0, tiled=True),)
    else:
        spectra = spectra.reshape(radix, 3, height, LANES // width, width)
        spectra = jnp.transpose(spectra, (0, 3, 1, 2, 4)).reshape(bands * count, -1)
        spectra = lax.all_to_all(spectra, axes, 0, 0, tiled=True)
        spectra = jnp.transpose(spectra.reshape(bands, count, 3, height, width), (2, 0, 1, 3, 4))
        spectra = spectra.reshape(3, bands, row_count, width)
        rest = jnp.zeros((bands, row_count, LANES - 2 * width), jnp.float32)
        spectra = (
            jnp.concatenate([spectra[0], spectra[1], rest], axis=2),
            jnp.concatenate([spectra[2], spectra[2], rest], axis=2),
        )
    advanced = call(
        lambda *refs: advance_kernel(packed, count, *refs),
        float_shape(bands * count, 2 * SUBLANES, LANES) if packed else float_shape(bands, row_count, LANES),
        [VMEM] * (len(spectra) + 6),
        (*spectra, growth, forcing, high, low, high_t, low_t),
    )
    if packed:
        advanced = lax.all_to_all(advanced, axes, 0, 0, tiled=True)
    else:
        advanced = advanced[:, :, : 2 * width].reshape(bands, count, height, 2, width)
        advanced = jnp.transpose(advanced, (0, 1, 3, 2, 4)).reshape(bands * count, -1)
        advanced = lax.all_to_all(advanced, axes, 0, 0, tiled=True)
        advanced = jnp.transpose(advanced.reshape(radix, LANES // width, 2, height, width), (0, 2, 3, 1, 4))
        advanced = advanced.reshape(radix, 2 * height, LANES)
    shift = FEED_RATE * math.expm1(-FEED_RATE * 0.5 * TIME_STEP) / -FEED_RATE
    values = call(
        lambda *refs: inverse_kernel(packed, count, shift, *refs),
        float_shape(count, 2, height, col_count),
        [SMEM] + [VMEM] * 3,
        (places, advanced, high_t, low_t),
    )
    blocks = swap_blocks([values[step] for step in range(count)])
    out = jnp.zeros((2, count, height, col_count), jnp.float32)
    for step, block in enumerate(blocks):
        out = lax.dynamic_update_index_in_dim(out, block, place ^ step, 1)
    out = out.reshape(2, row_count, col_count)
    return (out[0], out[1])


def solution(mesh):
    in_specs = (P("row", "col"), P("row", "col"))
    out_specs = (P("row", "col"), P("row", "col"))
    return jax.shard_map(
        on_device, mesh=mesh, in_specs=in_specs, out_specs=out_specs, check_vma=False
    )
```

```python
import math

import jax
import jax.numpy as jnp
import numpy as np
from jax import lax
from jax.experimental import pallas as pl
from jax.experimental.pallas import tpu as pltpu
from jax.sharding import PartitionSpec as P

FEED_RATE = 0.037
KILL_RATE = 0.06
TIME_STEP = 8.0
SUBSTRATE_DIFFUSION = 4e-07
ACTIVATOR_DIFFUSION = 2e-07
LANES = 128
SUBLANES = 8
VMEM_LIMIT = 36 << 20
VMEM = pl.BlockSpec(memory_space=pltpu.VMEM)
HBM = pl.BlockSpec(memory_space=pltpu.HBM)
SMEM = pl.BlockSpec(memory_space=pltpu.SMEM)


def basis_matrices(total):
    radix = total // LANES
    b = np.arange(LANES, dtype=np.int64)[:, None]
    k2 = np.arange(LANES, dtype=np.int64)[None, :]

    def angles(k1):
        return (b * (k1 + radix * k2) % total) * (2.0 * np.pi / total)

    matrices = np.zeros((radix // 2, 2 * LANES, 2 * LANES))
    for half, k1 in enumerate((0, radix // 2)):
        theta = angles(k1)
        part = slice(half * LANES, (half + 1) * LANES)
        matrices[0, part, part] = np.cos(theta) + np.sin(theta)
    for k1 in range(1, radix // 2):
        cosine, sine = np.cos(angles(k1)), np.sin(angles(k1))
        matrices[k1] = np.block([[cosine, -sine], [sine, cosine]])
    return matrices


def split_constant(matrices):
    high = matrices.astype(jnp.bfloat16)
    low = (matrices - high.astype(np.float64)).astype(jnp.bfloat16)
    return jnp.asarray(np.stack([high, low]))


def split_value(values):
    high = values.astype(jnp.bfloat16)
    low = (values - high.astype(jnp.float32)).astype(jnp.bfloat16)
    return high, low


def dot(left, right):
    return jnp.dot(left, right, preferred_element_type=jnp.float32)


def dot_pairs(left, right):
    return dot(left[0], right[0]) + (dot(left[0], right[1]) + dot(left[1], right[0]))


def turn(value, k, period, sign):
    real, imag = value
    if k == 0:
        return value
    if 4 * k == period:
        return (-sign * imag, sign * real) if imag is not None else (None, sign * real)
    cosine, sine = math.cos(2.0 * math.pi * k / period), sign * math.sin(2.0 * math.pi * k / period)
    if imag is None:
        return (real * cosine, real * sine)
    if 8 * k == period:
        return ((real - sign * imag) * cosine, (imag + sign * real) * cosine)
    return (real * cosine - imag * sine, real * sine + imag * cosine)


def plus(left, right):
    if left is None or right is None:
        return left if right is None else right
    return left + right


def minus(left, right):
    if right is None:
        return left
    return -right if left is None else left - right


def real_dft(values):
    n = len(values)
    if n == 1:
        return [(values[0], None)]
    even, odd = real_dft(values[0::2]), real_dft(values[1::2])
    out = [None] * (n // 2 + 1)
    for k in range(n // 4 + 1):
        turned = turn(odd[k], k, n, -1.0)
        if n // 2 - k != k:
            out[n // 2 - k] = (minus(even[k][0], turned[0]), minus(turned[1], even[k][1]))
        out[k] = (plus(even[k][0], turned[0]), plus(even[k][1], turned[1]))
    return out


def real_dft_transposed(spectrum):
    n = 2 * (len(spectrum) - 1)
    if n == 0:
        return [spectrum[0][0]]
    even, odd = [], []
    for k in range(n // 4 + 1):
        near, far = spectrum[k], spectrum[n // 2 - k]
        if k == 0:
            even.append((near[0] + far[0], None))
            odd.append((near[0] - far[0], None))
        elif 4 * k == n:
            even.append((near[0], None))
            odd.append((-near[1], None))
        else:
            even.append((near[0] + far[0], near[1] - far[1]))
            odd.append(turn((near[0] - far[0], near[1] + far[1]), k, n, 1.0))
    out = [None] * n
    out[0::2] = real_dft_transposed(even)
    out[1::2] = real_dft_transposed(odd)
    return out


def paired(spectrum, axis):
    half = len(spectrum) - 1
    rows = [(spectrum[0][0], spectrum[half][0])] + spectrum[1:half]
    return [jnp.concatenate(row, axis=axis) for row in rows]


def unpaired(products, axis):
    def halves(value):
        return lax.slice_in_dim(value, 0, LANES, axis=axis), lax.slice_in_dim(value, LANES, 2 * LANES, axis=axis)

    parts = [halves(value) for value in products]
    first, last = parts[0]
    return [(first, None)] + parts[1:] + [(last, None)]


def lane_chunk(shape, width):
    return lax.broadcasted_iota(jnp.int32, shape, len(shape) - 1) // width


def pick_chunks(pieces, width):
    chunk = lane_chunk(pieces[0].shape, width)
    out = pieces[-1]
    for index in range(len(pieces) - 2, -1, -1):
        out = jnp.where(chunk == index, pieces[index], out)
    return out


def rolled(value, chunks, width):
    shift = chunks * width % LANES
    return pltpu.roll(value, shift, 1) if shift else value


def wave_squares(k1, k2, total):
    radix = total // LANES
    wave = k1 + radix * k2
    signed = jnp.where(2 * wave < total, wave, wave - total).astype(jnp.float32)
    angular = (2.0 * math.pi) * signed
    return angular * angular


def tables_kernel(total_rows, total_cols, width, device_ref, *refs):
    *matrix_refs, growth_ref, forcing_ref, loaded_ref, loaded_t_ref, semaphores = refs
    copies = [
        pltpu.make_async_copy(source, target, semaphores.at[index])
        for index, (source, target) in enumerate(zip(matrix_refs, (loaded_ref, loaded_t_ref)))
    ]
    for copy in copies:
        copy.start()
    radix = total_rows // LANES
    chunks = LANES // width
    device = device_ref[0]
    tile, place = device // chunks, device % chunks
    lane = lax.broadcasted_iota(jnp.int32, (1, LANES), 1)
    col_class = jnp.where(tile == 0, 0, jnp.where(tile == 1, total_cols // LANES // 2, tile // 2))
    col_squares = wave_squares(col_class, place * width + lane % width, total_cols)
    col_scale = jnp.where(tile < 2, 1.0 / total_cols, 2.0 / total_cols).astype(jnp.float32)
    first = lane < width
    diffusion = jnp.where(first, SUBSTRATE_DIFFUSION, ACTIVATOR_DIFFUSION).astype(jnp.float32)
    decay = jnp.where(first, FEED_RATE, FEED_RATE + KILL_RATE).astype(jnp.float32)
    sign = jnp.where(first, -1.0, 1.0).astype(jnp.float32)
    k2 = lax.broadcasted_iota(jnp.int32, (LANES, LANES), 0)
    for index in range(radix // 2):
        for half in range(2):
            k1 = half * (radix // 2) if index == 0 else index
            scale = col_scale * ((1.0 if index == 0 else 2.0) / total_rows)
            linear = -diffusion * (wave_squares(k1, k2, total_rows) + col_squares) - decay
            growth = jnp.exp(linear * (0.5 * TIME_STEP))
            rows = slice(half * LANES, (half + 1) * LANES)
            growth_ref[index, rows, :] = growth * scale
            forcing_ref[index, rows, :] = (growth - 1.0) / linear * (scale * sign)
    for copy in copies:
        copy.wait()


def forward_kernel(packed, place_ref, *refs):
    *block_refs, matrix_ref, out_ref, buffer_ref = refs
    count = len(block_refs)
    place = place_ref[0]
    for step, block_ref in enumerate(block_refs):
        buffer_ref[place ^ step] = block_ref[...]
    cols = buffer_ref.shape[-1]
    height = buffer_ref.shape[2]
    tiles = []
    for source in range(count):
        for tile in range(cols // LANES):
            part = slice(tile * LANES, (tile + 1) * LANES)
            substrate = buffer_ref[source, 0, :, part]
            activator = buffer_ref[source, 1, :, part]
            tiles.append(jnp.concatenate([substrate, activator, substrate * activator * activator], axis=0))
    operands = paired(real_dft(tiles), 1)
    for index, operand in enumerate(operands):
        product = dot_pairs(split_value(operand), (matrix_ref[0, index], matrix_ref[1, index]))
        for half in range(2):
            tile = 2 * index + half
            spectrum = product[:, half * LANES : (half + 1) * LANES]
            if not packed:
                out_ref[tile] = spectrum
                continue
            width = LANES // count
            turns = [rolled(spectrum, shift, width) for shift in range(count)]
            for chunk in range(count):
                for field in range(3):
                    base = field * height
                    pieces = [
                        turns[(group - chunk) % count][base + group * SUBLANES : base + (group + 1) * SUBLANES]
                        for group in range(count)
                    ]
                    out_ref[tile * count + chunk, field * SUBLANES : (field + 1) * SUBLANES, :] = pick_chunks(
                        pieces, width
                    )


def advance_kernel(packed, count, *refs):
    if packed:
        in_ref, growth_ref, forcing_ref, matrix_ref, matrix_t_ref, out_ref = refs
        width = LANES // count
        radix = in_ref.shape[0] // count
        tiles = []
        for band in range(radix):
            own_rows, source_rows = [], []
            for source in range(count):
                block = in_ref[band * count + source]
                turns = [
                    [rolled(block[field * SUBLANES : (field + 1) * SUBLANES], -shift, width) for shift in range(count)]
                    for field in range(3)
                ]
                low_half = lane_chunk((SUBLANES, LANES), width) == 0
                for group in range(count):
                    near, next_near = group, (group - 1) % count
                    own_rows.append(jnp.where(low_half, turns[0][near], turns[1][next_near]))
                    source_rows.append(jnp.where(low_half, turns[2][near], turns[2][next_near]))
            own = jnp.concatenate(own_rows, axis=0)
            tiles.append(jnp.concatenate([own, jnp.concatenate(source_rows, axis=0)], axis=1))
    else:
        own_ref, source_ref, growth_ref, forcing_ref, matrix_ref, matrix_t_ref, out_ref = refs
        radix = own_ref.shape[0]
        tiles = [jnp.concatenate([own_ref[band], source_ref[band]], axis=1) for band in range(radix)]
    operands = paired(real_dft(tiles), 0)
    products = []
    for index, operand in enumerate(operands):
        spectrum = dot_pairs((matrix_t_ref[0, index], matrix_t_ref[1, index]), split_value(operand))
        advanced = growth_ref[index] * spectrum[:, :LANES] + forcing_ref[index] * spectrum[:, LANES:]
        products.append(dot_pairs((matrix_ref[0, index], matrix_ref[1, index]), split_value(advanced)))
    bands = real_dft_transposed(unpaired(products, 0))
    for band, value in enumerate(bands):
        if not packed:
            out_ref[band] = value
            continue
        height = LANES // count
        for target in range(count):
            for field in range(2):
                pieces = [
                    rolled(
                        value[target * height + group * SUBLANES : target * height + (group + 1) * SUBLANES],
                        group - field,
                        width,
                    )
                    for group in range(count)
                ]
                out_ref[band * count + target, field * SUBLANES : (field + 1) * SUBLANES, :] = pick_chunks(
                    pieces, width
                )


def inverse_kernel(packed, count, shift, place_ref, in_ref, matrix_t_ref, *refs):
    place = place_ref[0]
    *out_refs, buffer_ref = refs
    radix = 2 * matrix_t_ref.shape[1]
    _, height, cols = out_refs[0].shape
    tiles = []
    for tile in range(radix):
        if not packed:
            tiles.append(in_ref[tile])
            continue
        width = LANES // count
        turns = [[rolled(in_ref[tile * count + chunk], step, width) for step in range(count)] for chunk in range(count)]
        rows = []
        for field in range(2):
            part = slice(field * SUBLANES, (field + 1) * SUBLANES)
            for group in range(count):
                rows.append(
                    pick_chunks([turns[chunk][(chunk - group) % count][part] for chunk in range(count)], width)
                )
        tiles.append(jnp.concatenate(rows, axis=0))
    products = []
    for index in range(radix // 2):
        operand = jnp.concatenate([tiles[2 * index], tiles[2 * index + 1]], axis=1)
        products.append(dot_pairs(split_value(operand), (matrix_t_ref[0, index], matrix_t_ref[1, index])))
    values = real_dft_transposed(unpaired(products, 1))
    per_target = cols // LANES
    for index, value in enumerate(values):
        target, tile = index // per_target, index % per_target
        part = slice(tile * LANES, (tile + 1) * LANES)
        buffer_ref[place ^ target, 0, :, part] = value[:height] + shift
        buffer_ref[place ^ target, 1, :, part] = value[height:]
    for step, out_ref in enumerate(out_refs):
        out_ref[...] = buffer_ref[step]


def start_all(copies):
    for copy in copies:
        copy.start()
    for copy in copies:
        copy.wait()


def cut_kernel(place_ref, *refs):
    *field_refs, semaphores = refs
    in_refs, out_refs = field_refs[:2], field_refs[2:]
    height = out_refs[0].shape[1]
    copies = []
    for step, out_ref in enumerate(out_refs):
        rows = pl.ds((place_ref[0] ^ step) * height, height)
        for field, in_ref in enumerate(in_refs):
            copies.append(pltpu.make_async_copy(in_ref.at[rows], out_ref.at[field], semaphores.at[step, field]))
    start_all(copies)


def join_kernel(place_ref, *refs):
    *block_refs, first_ref, second_ref, semaphores = refs
    height = block_refs[0].shape[1]
    copies = []
    for step, block_ref in enumerate(block_refs):
        rows = pl.ds((place_ref[0] ^ step) * height, height)
        for field, out_ref in enumerate((first_ref, second_ref)):
            copies.append(pltpu.make_async_copy(block_ref.at[field], out_ref.at[rows], semaphores.at[step, field]))
    start_all(copies)


def call(kernel, out_shape, specs, operands, scratch=(), out_spec=VMEM):
    return pl.pallas_call(
        kernel,
        out_shape=out_shape,
        in_specs=specs,
        out_specs=jax.tree.map(lambda _: out_spec, out_shape),
        scratch_shapes=list(scratch),
        compiler_params=pltpu.CompilerParams(vmem_limit_bytes=VMEM_LIMIT),
    )(*operands)


def in_hbm(value):
    return pltpu.with_memory_space_constraint(value, pltpu.HBM)


def float_shape(*shape):
    return jax.ShapeDtypeStruct(shape, jnp.float32)


def swap_blocks(blocks):
    count = len(blocks)
    return [blocks[0]] + [
        lax.ppermute(blocks[step], "col", [(s, s ^ step) for s in range(count)]) for step in range(1, count)
    ]


def on_device(substrate, activator):
    row_count, col_count = substrate.shape
    bands, count = lax.axis_size("row"), lax.axis_size("col")
    total_rows, total_cols = row_count * bands, col_count * count
    height = row_count // count
    radix = total_cols // LANES
    width = total_cols // (bands * count)
    assert row_count == LANES and total_rows == total_cols and count & (count - 1) == 0
    packed = height == SUBLANES * count and width * count == LANES
    place = lax.axis_index("col")
    places = place[None].astype(jnp.int32)
    devices = (lax.axis_index("row") * count + place)[None].astype(jnp.int32)
    matrices = basis_matrices(total_rows)
    forward = split_constant(matrices)
    backward = split_constant(np.swapaxes(matrices, 1, 2))

    block = float_shape(2, height, col_count)
    blocks = swap_blocks(
        call(
            cut_kernel,
            [block] * count,
            [SMEM] + [HBM] * 2,
            (places, in_hbm(substrate), in_hbm(activator)),
            [pltpu.SemaphoreType.DMA((count, 2))],
        )
    )
    growth, forcing, forward, backward = call(
        lambda *refs: tables_kernel(total_rows, total_cols, width, *refs),
        [float_shape(radix // 2, 2 * LANES, LANES)] * 2
        + [jax.ShapeDtypeStruct(constant.shape, constant.dtype) for constant in (forward, backward)],
        [SMEM, HBM, HBM],
        (devices, in_hbm(forward), in_hbm(backward)),
        [pltpu.SemaphoreType.DMA((2,))],
    )
    spectra = call(
        lambda *refs: forward_kernel(packed, *refs),
        float_shape(bands * count, 3 * SUBLANES, LANES) if packed else float_shape(radix, 3 * height, LANES),
        [SMEM] + [VMEM] * (count + 1),
        (places, *blocks, forward),
        [pltpu.VMEM((count, 2, height, col_count), jnp.float32)],
    )
    axes = ("row", "col")
    if packed:
        spectra = (lax.all_to_all(spectra, axes, 0, 0, tiled=True),)
    else:
        spectra = spectra.reshape(radix, 3, height, LANES // width, width)
        spectra = jnp.transpose(spectra, (0, 3, 1, 2, 4)).reshape(bands * count, -1)
        spectra = lax.all_to_all(spectra, axes, 0, 0, tiled=True)
        spectra = jnp.transpose(spectra.reshape(bands, count, 3, height, width), (2, 0, 1, 3, 4))
        spectra = spectra.reshape(3, bands, row_count, width)
        rest = jnp.zeros((bands, row_count, LANES - 2 * width), jnp.float32)
        spectra = (
            jnp.concatenate([spectra[0], spectra[1], rest], axis=2),
            jnp.concatenate([spectra[2], spectra[2], rest], axis=2),
        )
    advanced = call(
        lambda *refs: advance_kernel(packed, count, *refs),
        float_shape(bands * count, 2 * SUBLANES, LANES) if packed else float_shape(bands, row_count, LANES),
        [VMEM] * (len(spectra) + 4),
        (*spectra, growth, forcing, forward, backward),
    )
    if packed:
        advanced = lax.all_to_all(advanced, axes, 0, 0, tiled=True)
    else:
        advanced = advanced[:, :, : 2 * width].reshape(bands, count, height, 2, width)
        advanced = jnp.transpose(advanced, (0, 1, 3, 2, 4)).reshape(bands * count, -1)
        advanced = lax.all_to_all(advanced, axes, 0, 0, tiled=True)
        advanced = jnp.transpose(advanced.reshape(radix, LANES // width, 2, height, width), (0, 2, 3, 1, 4))
        advanced = advanced.reshape(radix, 2 * height, LANES)
    shift = FEED_RATE * math.expm1(-FEED_RATE * 0.5 * TIME_STEP) / -FEED_RATE
    blocks = swap_blocks(
        call(
            lambda *refs: inverse_kernel(packed, count, shift, *refs),
            [block] * count,
            [SMEM] + [VMEM] * 2,
            (places, advanced, backward),
            [pltpu.VMEM((count, 2, height, col_count), jnp.float32)],
        )
    )
    return tuple(
        call(
            join_kernel,
            [float_shape(row_count, col_count)] * 2,
            [SMEM] + [VMEM] * count,
            (places, *blocks),
            [pltpu.SemaphoreType.DMA((count, 2))],
            HBM,
        )
    )


def solution(mesh):
    in_specs = (P("row", "col"), P("row", "col"))
    out_specs = (P("row", "col"), P("row", "col"))
    return jax.shard_map(
        on_device, mesh=mesh, in_specs=in_specs, out_specs=out_specs, check_vma=False
    )
```

```python
import math

import jax
import jax.numpy as jnp
import numpy as np
from jax import lax
from jax.experimental import pallas as pl
from jax.experimental.pallas import tpu as pltpu
from jax.sharding import Mesh
from jax.sharding import PartitionSpec as P

FEED_RATE = 0.037
KILL_RATE = 0.06
TIME_STEP = 8.0
SUBSTRATE_DIFFUSION = 4e-07
ACTIVATOR_DIFFUSION = 2e-07
LANES = 128
HALF = LANES // 2
CORES = 2
SUBLANES = 8
VMEM_LIMIT = 36 << 20
VMEM = pl.BlockSpec(memory_space=pltpu.VMEM)
HBM = pl.BlockSpec(memory_space=pltpu.HBM)
SMEM = pl.BlockSpec(memory_space=pltpu.SMEM)


def basis_matrices(total):
    radix = total // LANES
    b = np.arange(LANES, dtype=np.int64)[:, None]
    k2 = np.arange(LANES, dtype=np.int64)[None, :]

    def angles(k1):
        return (b * (k1 + radix * k2) % total) * (2.0 * np.pi / total)

    matrices = np.zeros((radix // 2, 2 * LANES, 2 * LANES))
    for half, k1 in enumerate((0, radix // 2)):
        theta = angles(k1)
        part = slice(half * LANES, (half + 1) * LANES)
        matrices[0, part, part] = np.cos(theta) + np.sin(theta)
    for k1 in range(1, radix // 2):
        cosine, sine = np.cos(angles(k1)), np.sin(angles(k1))
        matrices[k1] = np.block([[cosine, -sine], [sine, cosine]])
    return matrices


def split_constant(matrices):
    high = matrices.astype(jnp.bfloat16)
    low = (matrices - high.astype(np.float64)).astype(jnp.bfloat16)
    return jnp.asarray(np.stack([high, low]))


def split_value(values):
    high = values.astype(jnp.bfloat16)
    low = (values - high.astype(jnp.float32)).astype(jnp.bfloat16)
    return high, low


def dot(left, right):
    return jnp.dot(left, right, preferred_element_type=jnp.float32)


def dot_pairs(left, right):
    return dot(left[0], right[0]) + (dot(left[0], right[1]) + dot(left[1], right[0]))


def turn(value, k, period, sign):
    real, imag = value
    if k == 0:
        return value
    if 4 * k == period:
        return (-sign * imag, sign * real) if imag is not None else (None, sign * real)
    cosine, sine = math.cos(2.0 * math.pi * k / period), sign * math.sin(2.0 * math.pi * k / period)
    if imag is None:
        return (real * cosine, real * sine)
    if 8 * k == period:
        return ((real - sign * imag) * cosine, (imag + sign * real) * cosine)
    return (real * cosine - imag * sine, real * sine + imag * cosine)


def plus(left, right):
    if left is None or right is None:
        return left if right is None else right
    return left + right


def minus(left, right):
    if right is None:
        return left
    return -right if left is None else left - right


def real_dft(values):
    n = len(values)
    if n == 1:
        return [(values[0], None)]
    even, odd = real_dft(values[0::2]), real_dft(values[1::2])
    out = [None] * (n // 2 + 1)
    for k in range(n // 4 + 1):
        turned = turn(odd[k], k, n, -1.0)
        if n // 2 - k != k:
            out[n // 2 - k] = (minus(even[k][0], turned[0]), minus(turned[1], even[k][1]))
        out[k] = (plus(even[k][0], turned[0]), plus(even[k][1], turned[1]))
    return out


def real_dft_transposed(spectrum):
    n = 2 * (len(spectrum) - 1)
    if n == 0:
        return [spectrum[0][0]]
    even, odd = [], []
    for k in range(n // 4 + 1):
        near, far = spectrum[k], spectrum[n // 2 - k]
        if k == 0:
            even.append((near[0] + far[0], None))
            odd.append((near[0] - far[0], None))
        elif 4 * k == n:
            even.append((near[0], None))
            odd.append((-near[1], None))
        else:
            even.append((near[0] + far[0], near[1] - far[1]))
            odd.append(turn((near[0] - far[0], near[1] + far[1]), k, n, 1.0))
    out = [None] * n
    out[0::2] = real_dft_transposed(even)
    out[1::2] = real_dft_transposed(odd)
    return out


def paired(spectrum, axis):
    half = len(spectrum) - 1
    rows = [(spectrum[0][0], spectrum[half][0])] + spectrum[1:half]
    return [jnp.concatenate(row, axis=axis) for row in rows]


def unpaired(products, axis):
    def halves(value):
        return lax.slice_in_dim(value, 0, LANES, axis=axis), lax.slice_in_dim(value, LANES, 2 * LANES, axis=axis)

    parts = [halves(value) for value in products]
    first, last = parts[0]
    return [(first, None)] + parts[1:] + [(last, None)]


def lane_chunk(shape, width):
    return lax.broadcasted_iota(jnp.int32, shape, len(shape) - 1) // width


def pick_chunks(pieces, width):
    chunk = lane_chunk(pieces[0].shape, width)
    out = pieces[-1]
    for index in range(len(pieces) - 2, -1, -1):
        out = jnp.where(chunk == index, pieces[index], out)
    return out


def rolled(value, chunks, width):
    shift = chunks * width % LANES
    return pltpu.roll(value, shift, 1) if shift else value


def wave_squares(k1, k2, total):
    radix = total // LANES
    wave = k1 + radix * k2
    signed = jnp.where(2 * wave < total, wave, wave - total).astype(jnp.float32)
    angular = (2.0 * math.pi) * signed
    return angular * angular


def tables_kernel(total_rows, total_cols, width, device_ref, *refs):
    *matrix_refs, table_ref, loaded_ref, loaded_t_ref, semaphores = refs
    copies = [
        pltpu.make_async_copy(source, target, semaphores.at[index])
        for index, (source, target) in enumerate(zip(matrix_refs, (loaded_ref, loaded_t_ref)))
    ]
    for copy in copies:
        copy.start()
    radix = total_rows // LANES
    chunks = LANES // width
    device = device_ref[0]
    tile, place = device // chunks, device % chunks
    lane = lax.broadcasted_iota(jnp.int32, (1, LANES), 1)
    col_class = jnp.where(tile == 0, 0, jnp.where(tile == 1, total_cols // LANES // 2, tile // 2))
    col_squares = wave_squares(col_class, place * width + lane % width, total_cols)
    col_scale = jnp.where(tile < 2, 1.0 / total_cols, 2.0 / total_cols).astype(jnp.float32)
    first = lane % HALF < width
    diffusion = jnp.where(first, SUBSTRATE_DIFFUSION, ACTIVATOR_DIFFUSION).astype(jnp.float32)
    decay = jnp.where(first, FEED_RATE, FEED_RATE + KILL_RATE).astype(jnp.float32)
    sign = jnp.where(first, -1.0, 1.0).astype(jnp.float32)
    k2 = lax.broadcasted_iota(jnp.int32, (LANES, LANES), 0)
    for index in range(radix // 2):
        for half in range(2):
            k1 = half * (radix // 2) if index == 0 else index
            scale = col_scale * ((1.0 if index == 0 else 2.0) / total_rows)
            linear = -diffusion * (wave_squares(k1, k2, total_rows) + col_squares) - decay
            growth = jnp.exp(linear * (0.5 * TIME_STEP))
            rows = slice(half * LANES, (half + 1) * LANES)
            forcing = (growth - 1.0) / linear * sign
            table_ref[index, rows, :] = jnp.where(lane < HALF, growth, forcing) * scale
    for copy in copies:
        copy.wait()


def forward_kernel(packed, place_ref, *refs):
    *block_refs, matrix_ref, out_ref, buffer_ref = refs
    count = len(block_refs)
    place = place_ref[0]
    for step, block_ref in enumerate(block_refs):
        buffer_ref[place ^ step] = block_ref[...]
    cols = buffer_ref.shape[-1]
    height = buffer_ref.shape[2]
    tiles = []
    for source in range(count):
        for tile in range(cols // LANES):
            part = slice(tile * LANES, (tile + 1) * LANES)
            substrate = buffer_ref[source, 0, :, part]
            activator = buffer_ref[source, 1, :, part]
            tiles.append(jnp.concatenate([substrate, activator, substrate * activator * activator], axis=0))
    operands = paired(real_dft(tiles), 1)
    for index, operand in enumerate(operands):
        product = dot_pairs(split_value(operand), (matrix_ref[0, index], matrix_ref[1, index]))
        for half in range(2):
            tile = 2 * index + half
            spectrum = product[:, half * LANES : (half + 1) * LANES]
            if not packed:
                out_ref[tile] = spectrum
                continue
            width = LANES // count
            turns = [rolled(spectrum, shift, width) for shift in range(count)]
            for chunk in range(count):
                for field in range(3):
                    base = field * height
                    pieces = [
                        turns[(group - chunk) % count][base + group * SUBLANES : base + (group + 1) * SUBLANES]
                        for group in range(count)
                    ]
                    out_ref[tile * count + chunk, field * SUBLANES : (field + 1) * SUBLANES, :] = pick_chunks(
                        pieces, width
                    )


def place_of(band, source, bands):
    return (source * CORES + band % CORES) * (bands // CORES) + band // CORES


def advance_kernel(packed, count, in_ref, table_ref, matrix_ref, matrix_t_ref, out_ref):
    if packed:
        width = LANES // count
        radix = in_ref.shape[0] // count
        tiles = []
        for band in range(radix):
            rows = []
            for source in range(count):
                block = in_ref[place_of(band, source, radix)]
                turns = [
                    [rolled(block[field * SUBLANES : (field + 1) * SUBLANES], shift, width) for shift in range(count)]
                    for field in range(3)
                ]
                for group in range(count):
                    rows.append(
                        pick_chunks(
                            [turns[min(place, 2)][(place - group) % count] for place in range(count)], width
                        )
                    )
            tiles.append(jnp.concatenate(rows, axis=0))
    else:
        radix = in_ref.shape[0]
        tiles = [in_ref[band] for band in range(radix)]
    operands = paired(real_dft(tiles), 0)
    low_half = lax.broadcasted_iota(jnp.int32, (2 * LANES, LANES), 1) < HALF
    products = []
    for index, operand in enumerate(operands):
        high, low = split_value(operand)
        both = dot(matrix_t_ref[0, index], jnp.concatenate([high, low], axis=1))
        spectrum = both[:, :LANES] + (both[:, LANES:] + dot(matrix_t_ref[1, index], high))
        scaled = table_ref[index] * spectrum
        advanced = scaled + pltpu.roll(scaled, HALF, 1)
        high = advanced.astype(jnp.bfloat16).astype(jnp.float32)
        both = dot(matrix_ref[0, index], jnp.where(low_half, high, advanced - high).astype(jnp.bfloat16))
        rest = dot(matrix_ref[1, index], high.astype(jnp.bfloat16))
        products.append(both + (pltpu.roll(both, HALF, 1) + rest))
    bands = real_dft_transposed(unpaired(products, 0))
    for band, value in enumerate(bands):
        if not packed:
            out_ref[band] = value
            continue
        height = LANES // count
        for target in range(count):
            for field in range(2):
                pieces = [
                    rolled(
                        value[target * height + group * SUBLANES : target * height + (group + 1) * SUBLANES],
                        group - field,
                        width,
                    )
                    for group in range(count)
                ]
                out_ref[place_of(band, target, radix), field * SUBLANES : (field + 1) * SUBLANES, :] = pick_chunks(
                    pieces, width
                )


def inverse_kernel(packed, count, shift, place_ref, in_ref, matrix_t_ref, *refs):
    place = place_ref[0]
    *out_refs, buffer_ref = refs
    radix = 2 * matrix_t_ref.shape[1]
    _, height, cols = out_refs[0].shape
    tiles = []
    for tile in range(radix):
        if not packed:
            tiles.append(in_ref[tile])
            continue
        width = LANES // count
        turns = [[rolled(in_ref[tile * count + chunk], step, width) for step in range(count)] for chunk in range(count)]
        rows = []
        for field in range(2):
            part = slice(field * SUBLANES, (field + 1) * SUBLANES)
            for group in range(count):
                rows.append(
                    pick_chunks([turns[chunk][(chunk - group) % count][part] for chunk in range(count)], width)
                )
        tiles.append(jnp.concatenate(rows, axis=0))
    products = []
    for index in range(radix // 2):
        operand = jnp.concatenate([tiles[2 * index], tiles[2 * index + 1]], axis=1)
        products.append(dot_pairs(split_value(operand), (matrix_t_ref[0, index], matrix_t_ref[1, index])))
    values = real_dft_transposed(unpaired(products, 1))
    per_target = cols // LANES
    for index, value in enumerate(values):
        target, tile = index // per_target, index % per_target
        part = slice(tile * LANES, (tile + 1) * LANES)
        buffer_ref[place ^ target, 0, :, part] = value[:height] + shift
        buffer_ref[place ^ target, 1, :, part] = value[height:]
    for step, out_ref in enumerate(out_refs):
        out_ref[...] = buffer_ref[step]


def start_all(copies):
    for copy in copies:
        copy.start()
    for copy in copies:
        copy.wait()


def cut_kernel(place_ref, *refs):
    *field_refs, semaphores = refs
    in_refs, out_refs = field_refs[:2], field_refs[2:]
    height = out_refs[0].shape[1]
    copies = []
    for step, out_ref in enumerate(out_refs):
        rows = pl.ds((place_ref[0] ^ step) * height, height)
        for field, in_ref in enumerate(in_refs):
            copies.append(pltpu.make_async_copy(in_ref.at[rows], out_ref.at[field], semaphores.at[step, field]))
    start_all(copies)


def join_kernel(place_ref, *refs):
    *block_refs, first_ref, second_ref, semaphores = refs
    height = block_refs[0].shape[1]
    copies = []
    for step, block_ref in enumerate(block_refs):
        rows = pl.ds((place_ref[0] ^ step) * height, height)
        for field, out_ref in enumerate((first_ref, second_ref)):
            copies.append(pltpu.make_async_copy(block_ref.at[field], out_ref.at[rows], semaphores.at[step, field]))
    start_all(copies)


def call(kernel, out_shape, specs, operands, scratch=(), out_spec=VMEM):
    return pl.pallas_call(
        kernel,
        out_shape=out_shape,
        in_specs=specs,
        out_specs=jax.tree.map(lambda _: out_spec, out_shape),
        scratch_shapes=list(scratch),
        compiler_params=pltpu.CompilerParams(vmem_limit_bytes=VMEM_LIMIT),
    )(*operands)


def in_hbm(value):
    return pltpu.with_memory_space_constraint(value, pltpu.HBM)


def float_shape(*shape):
    return jax.ShapeDtypeStruct(shape, jnp.float32)


def swap_blocks(blocks):
    count = len(blocks)
    return [blocks[0]] + [
        lax.ppermute(blocks[step], "col", [(s, s ^ step) for s in range(count)]) for step in range(1, count)
    ]


def on_device(substrate, activator):
    row_count, col_count = substrate.shape
    bands, count = lax.axis_size("outer") * lax.axis_size("core"), lax.axis_size("col")
    total_rows, total_cols = row_count * bands, col_count * count
    height = row_count // count
    radix = total_cols // LANES
    width = total_cols // (bands * count)
    assert row_count == LANES and total_rows == total_cols and count & (count - 1) == 0
    packed = height == SUBLANES * count and width * count == LANES
    place = lax.axis_index("col")
    places = place[None].astype(jnp.int32)
    axes = ("col", "core", "outer")
    devices = lax.axis_index(axes)[None].astype(jnp.int32)
    matrices = basis_matrices(total_rows)
    forward = split_constant(matrices)
    backward = split_constant(np.swapaxes(matrices, 1, 2))

    block = float_shape(2, height, col_count)
    blocks = swap_blocks(
        call(
            cut_kernel,
            [block] * count,
            [SMEM] + [HBM] * 2,
            (places, in_hbm(substrate), in_hbm(activator)),
            [pltpu.SemaphoreType.DMA((count, 2))],
        )
    )
    table, forward, backward = call(
        lambda *refs: tables_kernel(total_rows, total_cols, width, *refs),
        [float_shape(radix // 2, 2 * LANES, LANES)]
        + [jax.ShapeDtypeStruct(constant.shape, constant.dtype) for constant in (forward, backward)],
        [SMEM, HBM, HBM],
        (devices, in_hbm(forward), in_hbm(backward)),
        [pltpu.SemaphoreType.DMA((2,))],
    )
    spectra = call(
        lambda *refs: forward_kernel(packed, *refs),
        float_shape(bands * count, 3 * SUBLANES, LANES) if packed else float_shape(radix, 3 * height, LANES),
        [SMEM] + [VMEM] * (count + 1),
        (places, *blocks, forward),
        [pltpu.VMEM((count, 2, height, col_count), jnp.float32)],
    )
    if packed:
        spectra = lax.all_to_all(spectra, axes, 0, 0, tiled=True)
    else:
        spectra = spectra.reshape(radix, 3, height, LANES // width, width)
        spectra = jnp.transpose(spectra, (0, 3, 1, 2, 4)).reshape(bands * count, -1)
        spectra = lax.all_to_all(spectra, axes, 0, 0, tiled=True)
        spectra = spectra.reshape(count, CORES, bands // CORES, 3, height, width)
        spectra = jnp.transpose(spectra, (3, 2, 1, 0, 4, 5))
        spectra = spectra.reshape(3, bands, row_count, width)
        rest = jnp.zeros((bands, row_count, HALF - 2 * width), jnp.float32)
        spectra = jnp.concatenate([spectra[0], spectra[1], rest, spectra[2], spectra[2], rest], axis=2)
    advanced = call(
        lambda *refs: advance_kernel(packed, count, *refs),
        float_shape(bands * count, 2 * SUBLANES, LANES) if packed else float_shape(bands, row_count, LANES),
        [VMEM] * 4,
        (spectra, table, forward, backward),
    )
    if packed:
        advanced = lax.all_to_all(advanced, axes, 0, 0, tiled=True)
    else:
        advanced = advanced[:, :, : 2 * width].reshape(bands // CORES, CORES, count, height, 2, width)
        advanced = jnp.transpose(advanced, (2, 1, 0, 4, 3, 5)).reshape(bands * count, -1)
        advanced = lax.all_to_all(advanced, axes, 0, 0, tiled=True)
        advanced = jnp.transpose(advanced.reshape(radix, LANES // width, 2, height, width), (0, 2, 3, 1, 4))
        advanced = advanced.reshape(radix, 2 * height, LANES)
    shift = FEED_RATE * math.expm1(-FEED_RATE * 0.5 * TIME_STEP) / -FEED_RATE
    blocks = swap_blocks(
        call(
            lambda *refs: inverse_kernel(packed, count, shift, *refs),
            [block] * count,
            [SMEM] + [VMEM] * 2,
            (places, advanced, backward),
            [pltpu.VMEM((count, 2, height, col_count), jnp.float32)],
        )
    )
    return tuple(
        call(
            join_kernel,
            [float_shape(row_count, col_count)] * 2,
            [SMEM] + [VMEM] * count,
            (places, *blocks),
            [pltpu.SemaphoreType.DMA((count, 2))],
            HBM,
        )
    )


def solution(mesh):
    bands, count = mesh.shape["row"], mesh.shape["col"]
    split = Mesh(mesh.devices.reshape(bands // CORES, CORES, count), ("outer", "core", "col"))
    spec = P(("outer", "core"), "col")
    return jax.shard_map(on_device, mesh=split, in_specs=(spec, spec), out_specs=(spec, spec), check_vma=False)
```

```python
import math

import jax
import jax.numpy as jnp
import numpy as np
from jax import lax
from jax.experimental import pallas as pl
from jax.experimental.pallas import tpu as pltpu
from jax.sharding import Mesh
from jax.sharding import PartitionSpec as P

FEED_RATE = 0.037
KILL_RATE = 0.06
TIME_STEP = 8.0
SUBSTRATE_DIFFUSION = 4e-07
ACTIVATOR_DIFFUSION = 2e-07
LANES = 128
HALF = LANES // 2
CORES = 2
SUBLANES = 8
VMEM_LIMIT = 36 << 20
VMEM = pl.BlockSpec(memory_space=pltpu.VMEM)
HBM = pl.BlockSpec(memory_space=pltpu.HBM)
SMEM = pl.BlockSpec(memory_space=pltpu.SMEM)


def basis_matrices(total):
    radix = total // LANES
    b = np.arange(LANES, dtype=np.int64)[:, None]
    k2 = np.arange(LANES, dtype=np.int64)[None, :]

    def angles(k1):
        return (b * (k1 + radix * k2) % total) * (2.0 * np.pi / total)

    matrices = np.zeros((radix // 2, 2 * LANES, 2 * LANES))
    for half, k1 in enumerate((0, radix // 2)):
        theta = angles(k1)
        part = slice(half * LANES, (half + 1) * LANES)
        matrices[0, part, part] = np.cos(theta) + np.sin(theta)
    for k1 in range(1, radix // 2):
        cosine, sine = np.cos(angles(k1)), np.sin(angles(k1))
        matrices[k1] = np.block([[cosine, -sine], [sine, cosine]])
    return matrices


def split_constant(matrices):
    high = matrices.astype(jnp.bfloat16)
    low = (matrices - high.astype(np.float64)).astype(jnp.bfloat16)
    return jnp.asarray(np.stack([high, low]))


def split_value(values):
    high = values.astype(jnp.bfloat16)
    low = (values - high.astype(jnp.float32)).astype(jnp.bfloat16)
    return high, low


def dot(left, right):
    return jnp.dot(left, right, preferred_element_type=jnp.float32)


def dot_pairs(left, right):
    return dot(left[0], right[0]) + (dot(left[0], right[1]) + dot(left[1], right[0]))


def turn(value, k, period, sign):
    real, imag = value
    if k == 0:
        return value
    if 4 * k == period:
        return (-sign * imag, sign * real) if imag is not None else (None, sign * real)
    cosine, sine = math.cos(2.0 * math.pi * k / period), sign * math.sin(2.0 * math.pi * k / period)
    if imag is None:
        return (real * cosine, real * sine)
    if 8 * k == period:
        return ((real - sign * imag) * cosine, (imag + sign * real) * cosine)
    return (real * cosine - imag * sine, real * sine + imag * cosine)


def plus(left, right):
    if left is None or right is None:
        return left if right is None else right
    return left + right


def minus(left, right):
    if right is None:
        return left
    return -right if left is None else left - right


def real_dft(values):
    n = len(values)
    if n == 1:
        return [(values[0], None)]
    even, odd = real_dft(values[0::2]), real_dft(values[1::2])
    out = [None] * (n // 2 + 1)
    for k in range(n // 4 + 1):
        turned = turn(odd[k], k, n, -1.0)
        if n // 2 - k != k:
            out[n // 2 - k] = (minus(even[k][0], turned[0]), minus(turned[1], even[k][1]))
        out[k] = (plus(even[k][0], turned[0]), plus(even[k][1], turned[1]))
    return out


def real_dft_transposed(spectrum):
    n = 2 * (len(spectrum) - 1)
    if n == 0:
        return [spectrum[0][0]]
    even, odd = [], []
    for k in range(n // 4 + 1):
        near, far = spectrum[k], spectrum[n // 2 - k]
        if k == 0:
            even.append((near[0] + far[0], None))
            odd.append((near[0] - far[0], None))
        elif 4 * k == n:
            even.append((near[0], None))
            odd.append((-near[1], None))
        else:
            even.append((near[0] + far[0], near[1] - far[1]))
            odd.append(turn((near[0] - far[0], near[1] + far[1]), k, n, 1.0))
    out = [None] * n
    out[0::2] = real_dft_transposed(even)
    out[1::2] = real_dft_transposed(odd)
    return out


def paired(spectrum, axis):
    half = len(spectrum) - 1
    rows = [(spectrum[0][0], spectrum[half][0])] + spectrum[1:half]
    return [jnp.concatenate(row, axis=axis) for row in rows]


def unpaired(products, axis):
    def halves(value):
        return lax.slice_in_dim(value, 0, LANES, axis=axis), lax.slice_in_dim(value, LANES, 2 * LANES, axis=axis)

    parts = [halves(value) for value in products]
    first, last = parts[0]
    return [(first, None)] + parts[1:] + [(last, None)]


def lane_chunk(shape, width):
    return lax.broadcasted_iota(jnp.int32, shape, len(shape) - 1) // width


def swap_chunks(pieces):
    pieces = list(pieces)
    count = len(pieces)
    width = LANES // count
    chunk = lane_chunk(pieces[0].shape, width)
    step = count // 2
    while step:
        stays = chunk & step == 0
        for first in range(count):
            if first & step:
                continue
            near, far = pieces[first], pieces[first + step]
            pieces[first] = jnp.where(stays, near, pltpu.roll(far, step * width, 1))
            pieces[first + step] = jnp.where(stays, pltpu.roll(near, LANES - step * width, 1), far)
        step //= 2
    return pieces


def sublane_rows(value, group):
    return value[group * SUBLANES : (group + 1) * SUBLANES]


def wave_squares(k1, k2, total):
    radix = total // LANES
    wave = k1 + radix * k2
    signed = jnp.where(2 * wave < total, wave, wave - total).astype(jnp.float32)
    angular = (2.0 * math.pi) * signed
    return angular * angular


def tables_kernel(total_rows, total_cols, width, device_ref, *refs):
    *matrix_refs, table_ref, loaded_ref, loaded_t_ref, semaphores = refs
    copies = [
        pltpu.make_async_copy(source, target, semaphores.at[index])
        for index, (source, target) in enumerate(zip(matrix_refs, (loaded_ref, loaded_t_ref)))
    ]
    for copy in copies:
        copy.start()
    radix = total_rows // LANES
    chunks = LANES // width
    device = device_ref[0]
    tile, place = device // chunks, device % chunks
    lane = lax.broadcasted_iota(jnp.int32, (1, LANES), 1)
    col_class = jnp.where(tile == 0, 0, jnp.where(tile == 1, total_cols // LANES // 2, tile // 2))
    col_squares = wave_squares(col_class, place * width + lane % width, total_cols)
    col_scale = jnp.where(tile < 2, 1.0 / total_cols, 2.0 / total_cols).astype(jnp.float32)
    first = lane % HALF < width
    diffusion = jnp.where(first, SUBSTRATE_DIFFUSION, ACTIVATOR_DIFFUSION).astype(jnp.float32)
    decay = jnp.where(first, FEED_RATE, FEED_RATE + KILL_RATE).astype(jnp.float32)
    sign = jnp.where(first, -1.0, 1.0).astype(jnp.float32)
    k2 = lax.broadcasted_iota(jnp.int32, (LANES, LANES), 0)
    for index in range(radix // 2):
        for half in range(2):
            k1 = half * (radix // 2) if index == 0 else index
            scale = col_scale * ((1.0 if index == 0 else 2.0) / total_rows)
            linear = -diffusion * (wave_squares(k1, k2, total_rows) + col_squares) - decay
            growth = jnp.exp(linear * (0.5 * TIME_STEP))
            rows = slice(half * LANES, (half + 1) * LANES)
            forcing = (growth - 1.0) / linear * sign
            table_ref[index, rows, :] = jnp.where(lane < HALF, growth, forcing) * scale
    for copy in copies:
        copy.wait()


def forward_kernel(packed, place_ref, *refs):
    *block_refs, matrix_ref, out_ref, buffer_ref = refs
    count = len(block_refs)
    place = place_ref[0]
    for step, block_ref in enumerate(block_refs):
        buffer_ref[place ^ step] = block_ref[...]
    cols = buffer_ref.shape[-1]
    height = buffer_ref.shape[2]
    tiles = []
    for source in range(count):
        for tile in range(cols // LANES):
            part = slice(tile * LANES, (tile + 1) * LANES)
            substrate = buffer_ref[source, 0, :, part]
            activator = buffer_ref[source, 1, :, part]
            tiles.append(jnp.concatenate([substrate, activator, substrate * activator * activator], axis=0))
    operands = paired(real_dft(tiles), 1)
    for index, operand in enumerate(operands):
        product = dot_pairs(split_value(operand), (matrix_ref[0, index], matrix_ref[1, index]))
        for half in range(2):
            tile = 2 * index + half
            spectrum = product[:, half * LANES : (half + 1) * LANES]
            if not packed:
                out_ref[tile] = spectrum
                continue
            for field in range(3):
                part = spectrum[field * height : (field + 1) * height]
                for chunk, piece in enumerate(swap_chunks([sublane_rows(part, group) for group in range(count)])):
                    out_ref[tile * count + chunk, field * SUBLANES : (field + 1) * SUBLANES, :] = piece


def place_of(band, source, bands):
    return (source * CORES + band % CORES) * (bands // CORES) + band // CORES


def advance_kernel(packed, count, in_ref, table_ref, matrix_ref, matrix_t_ref, out_ref):
    if packed:
        radix = in_ref.shape[0] // count
        tiles = []
        for band in range(radix):
            rows = []
            for source in range(count):
                block = in_ref[place_of(band, source, radix)]
                rows += swap_chunks([sublane_rows(block, min(field, 2)) for field in range(count)])
            tiles.append(jnp.concatenate(rows, axis=0))
    else:
        radix = in_ref.shape[0]
        tiles = [in_ref[band] for band in range(radix)]
    operands = paired(real_dft(tiles), 0)
    low_half = lax.broadcasted_iota(jnp.int32, (2 * LANES, LANES), 1) < HALF
    scaled = []
    for index, operand in enumerate(operands):
        high, low = split_value(operand)
        both = dot(matrix_t_ref[0, index], jnp.concatenate([high, low], axis=1))
        spectrum = both[:, :LANES] + (both[:, LANES:] + dot(matrix_t_ref[1, index], high))
        scaled.append(table_ref[index] * spectrum)
    products = []
    for index, value in enumerate(scaled):
        advanced = value + pltpu.roll(value, HALF, 1)
        high = advanced.astype(jnp.bfloat16).astype(jnp.float32)
        both = dot(matrix_ref[0, index], jnp.where(low_half, high, advanced - high).astype(jnp.bfloat16))
        rest = dot(matrix_ref[1, index], high.astype(jnp.bfloat16))
        products.append(both + (pltpu.roll(both, HALF, 1) + rest))
    bands = real_dft_transposed(unpaired(products, 0))
    low_half = lane_chunk((SUBLANES, LANES), HALF) == 0
    even = lane_chunk((SUBLANES, LANES), HALF // 2) % 2 == 0
    for band, value in enumerate(bands):
        if not packed:
            out_ref[band] = value
            continue
        for target in range(count):
            part = value[target * LANES // count : (target + 1) * LANES // count]
            near = jnp.where(low_half, sublane_rows(part, 0), sublane_rows(part, 2))
            far = jnp.where(low_half, sublane_rows(part, 1), sublane_rows(part, 3))
            place = place_of(band, target, radix)
            out_ref[place, :SUBLANES, :] = jnp.where(even, near, pltpu.roll(far, HALF // 2, 1))
            out_ref[place, SUBLANES:, :] = jnp.where(even, pltpu.roll(near, LANES - HALF // 2, 1), far)


def inverse_kernel(packed, count, shift, place_ref, in_ref, matrix_t_ref, *refs):
    place = place_ref[0]
    *out_refs, buffer_ref = refs
    radix = 2 * matrix_t_ref.shape[1]
    _, height, cols = out_refs[0].shape
    tiles = []
    for tile in range(radix):
        if not packed:
            tiles.append(in_ref[tile])
            continue
        rows = []
        for field in range(2):
            rows += swap_chunks([sublane_rows(in_ref[tile * count + chunk], field) for chunk in range(count)])
        tiles.append(jnp.concatenate(rows, axis=0))
    products = []
    for index in range(radix // 2):
        operand = jnp.concatenate([tiles[2 * index], tiles[2 * index + 1]], axis=1)
        products.append(dot_pairs(split_value(operand), (matrix_t_ref[0, index], matrix_t_ref[1, index])))
    values = real_dft_transposed(unpaired(products, 1))
    per_target = cols // LANES
    for index, value in enumerate(values):
        target, tile = index // per_target, index % per_target
        part = slice(tile * LANES, (tile + 1) * LANES)
        buffer_ref[place ^ target, 0, :, part] = value[:height] + shift
        buffer_ref[place ^ target, 1, :, part] = value[height:]
    for step, out_ref in enumerate(out_refs):
        out_ref[...] = buffer_ref[step]


def start_all(copies):
    for copy in copies:
        copy.start()
    for copy in copies:
        copy.wait()


def cut_kernel(place_ref, *refs):
    *field_refs, semaphores = refs
    in_refs, out_refs = field_refs[:2], field_refs[2:]
    height = out_refs[0].shape[1]
    copies = []
    for step, out_ref in enumerate(out_refs):
        rows = pl.ds((place_ref[0] ^ step) * height, height)
        for field, in_ref in enumerate(in_refs):
            copies.append(pltpu.make_async_copy(in_ref.at[rows], out_ref.at[field], semaphores.at[step, field]))
    start_all(copies)


def join_kernel(place_ref, *refs):
    *block_refs, first_ref, second_ref, semaphores = refs
    height = block_refs[0].shape[1]
    copies = []
    for step, block_ref in enumerate(block_refs):
        rows = pl.ds((place_ref[0] ^ step) * height, height)
        for field, out_ref in enumerate((first_ref, second_ref)):
            copies.append(pltpu.make_async_copy(block_ref.at[field], out_ref.at[rows], semaphores.at[step, field]))
    start_all(copies)


def call(kernel, out_shape, specs, operands, scratch=(), out_spec=VMEM):
    return pl.pallas_call(
        kernel,
        out_shape=out_shape,
        in_specs=specs,
        out_specs=jax.tree.map(lambda _: out_spec, out_shape),
        scratch_shapes=list(scratch),
        compiler_params=pltpu.CompilerParams(vmem_limit_bytes=VMEM_LIMIT),
    )(*operands)


def in_hbm(value):
    return pltpu.with_memory_space_constraint(value, pltpu.HBM)


def float_shape(*shape):
    return jax.ShapeDtypeStruct(shape, jnp.float32)


def swap_blocks(blocks):
    count = len(blocks)
    return [blocks[0]] + [
        lax.ppermute(blocks[step], "col", [(s, s ^ step) for s in range(count)]) for step in range(1, count)
    ]


def on_device(substrate, activator):
    row_count, col_count = substrate.shape
    bands, count = lax.axis_size("outer") * lax.axis_size("core"), lax.axis_size("col")
    total_rows, total_cols = row_count * bands, col_count * count
    height = row_count // count
    radix = total_cols // LANES
    width = total_cols // (bands * count)
    assert row_count == LANES and total_rows == total_cols and count & (count - 1) == 0
    packed = count == 4 and height == SUBLANES * count and width * count == LANES
    place = lax.axis_index("col")
    places = place[None].astype(jnp.int32)
    axes = ("col", "core", "outer")
    devices = lax.axis_index(axes)[None].astype(jnp.int32)
    matrices = basis_matrices(total_rows)
    forward = split_constant(matrices)
    backward = split_constant(np.swapaxes(matrices, 1, 2))

    block = float_shape(2, height, col_count)
    blocks = swap_blocks(
        call(
            cut_kernel,
            [block] * count,
            [SMEM] + [HBM] * 2,
            (places, in_hbm(substrate), in_hbm(activator)),
            [pltpu.SemaphoreType.DMA((count, 2))],
        )
    )
    table, forward, backward = call(
        lambda *refs: tables_kernel(total_rows, total_cols, width, *refs),
        [float_shape(radix // 2, 2 * LANES, LANES)]
        + [jax.ShapeDtypeStruct(constant.shape, constant.dtype) for constant in (forward, backward)],
        [SMEM, HBM, HBM],
        (devices, in_hbm(forward), in_hbm(backward)),
        [pltpu.SemaphoreType.DMA((2,))],
    )
    spectra = call(
        lambda *refs: forward_kernel(packed, *refs),
        float_shape(bands * count, 3 * SUBLANES, LANES) if packed else float_shape(radix, 3 * height, LANES),
        [SMEM] + [VMEM] * (count + 1),
        (places, *blocks, forward),
        [pltpu.VMEM((count, 2, height, col_count), jnp.float32)],
    )
    if packed:
        spectra = lax.all_to_all(spectra, axes, 0, 0, tiled=True)
    else:
        spectra = spectra.reshape(radix, 3, height, LANES // width, width)
        spectra = jnp.transpose(spectra, (0, 3, 1, 2, 4)).reshape(bands * count, -1)
        spectra = lax.all_to_all(spectra, axes, 0, 0, tiled=True)
        spectra = spectra.reshape(count, CORES, bands // CORES, 3, height, width)
        spectra = jnp.transpose(spectra, (3, 2, 1, 0, 4, 5))
        spectra = spectra.reshape(3, bands, row_count, width)
        rest = jnp.zeros((bands, row_count, HALF - 2 * width), jnp.float32)
        spectra = jnp.concatenate([spectra[0], spectra[1], rest, spectra[2], spectra[2], rest], axis=2)
    advanced = call(
        lambda *refs: advance_kernel(packed, count, *refs),
        float_shape(bands * count, 2 * SUBLANES, LANES) if packed else float_shape(bands, row_count, LANES),
        [VMEM] * 4,
        (spectra, table, forward, backward),
    )
    if packed:
        advanced = lax.all_to_all(advanced, axes, 0, 0, tiled=True)
    else:
        advanced = advanced[:, :, : 2 * width].reshape(bands // CORES, CORES, count, height, 2, width)
        advanced = jnp.transpose(advanced, (2, 1, 0, 4, 3, 5)).reshape(bands * count, -1)
        advanced = lax.all_to_all(advanced, axes, 0, 0, tiled=True)
        advanced = jnp.transpose(advanced.reshape(radix, LANES // width, 2, height, width), (0, 2, 3, 1, 4))
        advanced = advanced.reshape(radix, 2 * height, LANES)
    shift = FEED_RATE * math.expm1(-FEED_RATE * 0.5 * TIME_STEP) / -FEED_RATE
    blocks = swap_blocks(
        call(
            lambda *refs: inverse_kernel(packed, count, shift, *refs),
            [block] * count,
            [SMEM] + [VMEM] * 2,
            (places, advanced, backward),
            [pltpu.VMEM((count, 2, height, col_count), jnp.float32)],
        )
    )
    return tuple(
        call(
            join_kernel,
            [float_shape(row_count, col_count)] * 2,
            [SMEM] + [VMEM] * count,
            (places, *blocks),
            [pltpu.SemaphoreType.DMA((count, 2))],
            HBM,
        )
    )


def solution(mesh):
    bands, count = mesh.shape["row"], mesh.shape["col"]
    split = Mesh(mesh.devices.reshape(bands // CORES, CORES, count), ("outer", "core", "col"))
    spec = P(("outer", "core"), "col")
    return jax.shard_map(on_device, mesh=split, in_specs=(spec, spec), out_specs=(spec, spec), check_vma=False)
```

```python
import math

import jax
import jax.numpy as jnp
import numpy as np
from jax import lax
from jax.experimental import pallas as pl
from jax.experimental.pallas import tpu as pltpu
from jax.sharding import Mesh
from jax.sharding import PartitionSpec as P

FEED_RATE = 0.037
KILL_RATE = 0.06
TIME_STEP = 8.0
SUBSTRATE_DIFFUSION = 4e-07
ACTIVATOR_DIFFUSION = 2e-07
LANES = 128
HALF = LANES // 2
CORES = 2
SUBLANES = 8
VMEM_LIMIT = 36 << 20
VMEM = pl.BlockSpec(memory_space=pltpu.VMEM)
HBM = pl.BlockSpec(memory_space=pltpu.HBM)
SMEM = pl.BlockSpec(memory_space=pltpu.SMEM)


def basis_matrices(total):
    radix = total // LANES
    b = np.arange(LANES, dtype=np.int64)[:, None]
    k2 = np.arange(LANES, dtype=np.int64)[None, :]

    def angles(k1):
        return (b * (k1 + radix * k2) % total) * (2.0 * np.pi / total)

    matrices = np.zeros((radix // 2, 2 * LANES, 2 * LANES))
    for half, k1 in enumerate((0, radix // 2)):
        theta = angles(k1)
        part = slice(half * LANES, (half + 1) * LANES)
        matrices[0, part, part] = np.cos(theta) + np.sin(theta)
    for k1 in range(1, radix // 2):
        cosine, sine = np.cos(angles(k1)), np.sin(angles(k1))
        matrices[k1] = np.block([[cosine, -sine], [sine, cosine]])
    return matrices


def split_constant(matrices):
    high = matrices.astype(jnp.bfloat16)
    low = (matrices - high.astype(np.float64)).astype(jnp.bfloat16)
    return jnp.asarray(np.stack([high, low]))


def split_value(values):
    high = values.astype(jnp.bfloat16)
    low = (values - high.astype(jnp.float32)).astype(jnp.bfloat16)
    return high, low


def dot(left, right):
    return jnp.dot(left, right, preferred_element_type=jnp.float32)


def dot_pairs(left, right):
    height = left[0].shape[0]
    both = dot(jnp.concatenate(left, axis=0), right[0])
    return both[:height] + (both[height:] + dot(left[0], right[1]))


def turn(value, k, period, sign):
    real, imag = value
    if k == 0:
        return value
    if 4 * k == period:
        return (-sign * imag, sign * real) if imag is not None else (None, sign * real)
    cosine, sine = math.cos(2.0 * math.pi * k / period), sign * math.sin(2.0 * math.pi * k / period)
    if imag is None:
        return (real * cosine, real * sine)
    if 8 * k == period:
        return ((real - sign * imag) * cosine, (imag + sign * real) * cosine)
    return (real * cosine - imag * sine, real * sine + imag * cosine)


def plus(left, right):
    if left is None or right is None:
        return left if right is None else right
    return left + right


def minus(left, right):
    if right is None:
        return left
    return -right if left is None else left - right


def real_dft(values):
    n = len(values)
    if n == 1:
        return [(values[0], None)]
    even, odd = real_dft(values[0::2]), real_dft(values[1::2])
    out = [None] * (n // 2 + 1)
    for k in range(n // 4 + 1):
        turned = turn(odd[k], k, n, -1.0)
        if n // 2 - k != k:
            out[n // 2 - k] = (minus(even[k][0], turned[0]), minus(turned[1], even[k][1]))
        out[k] = (plus(even[k][0], turned[0]), plus(even[k][1], turned[1]))
    return out


def real_dft_transposed(spectrum):
    n = 2 * (len(spectrum) - 1)
    if n == 0:
        return [spectrum[0][0]]
    even, odd = [], []
    for k in range(n // 4 + 1):
        near, far = spectrum[k], spectrum[n // 2 - k]
        if k == 0:
            even.append((near[0] + far[0], None))
            odd.append((near[0] - far[0], None))
        elif 4 * k == n:
            even.append((near[0], None))
            odd.append((-near[1], None))
        else:
            even.append((near[0] + far[0], near[1] - far[1]))
            odd.append(turn((near[0] - far[0], near[1] + far[1]), k, n, 1.0))
    out = [None] * n
    out[0::2] = real_dft_transposed(even)
    out[1::2] = real_dft_transposed(odd)
    return out


def paired(spectrum, axis):
    half = len(spectrum) - 1
    rows = [(spectrum[0][0], spectrum[half][0])] + spectrum[1:half]
    return [jnp.concatenate(row, axis=axis) for row in rows]


def unpaired(products, axis):
    def halves(value):
        return lax.slice_in_dim(value, 0, LANES, axis=axis), lax.slice_in_dim(value, LANES, 2 * LANES, axis=axis)

    parts = [halves(value) for value in products]
    first, last = parts[0]
    return [(first, None)] + parts[1:] + [(last, None)]


def lane_chunk(shape, width):
    return lax.broadcasted_iota(jnp.int32, shape, len(shape) - 1) // width


def swap_chunks(pieces):
    pieces = list(pieces)
    count = len(pieces)
    width = LANES // count
    chunk = lane_chunk(pieces[0].shape, width)
    step = count // 2
    while step:
        stays = chunk & step == 0
        for first in range(count):
            if first & step:
                continue
            near, far = pieces[first], pieces[first + step]
            pieces[first] = jnp.where(stays, near, pltpu.roll(far, step * width, 1))
            pieces[first + step] = jnp.where(stays, pltpu.roll(near, LANES - step * width, 1), far)
        step //= 2
    return pieces


def sublane_rows(value, group):
    return value[group * SUBLANES : (group + 1) * SUBLANES]


def wave_squares(k1, k2, total):
    radix = total // LANES
    wave = k1 + radix * k2
    signed = jnp.where(2 * wave < total, wave, wave - total).astype(jnp.float32)
    angular = (2.0 * math.pi) * signed
    return angular * angular


def tables_kernel(total_rows, total_cols, width, device_ref, *refs):
    *matrix_refs, table_ref, loaded_ref, loaded_t_ref, semaphores = refs
    copies = [
        pltpu.make_async_copy(source, target, semaphores.at[index])
        for index, (source, target) in enumerate(zip(matrix_refs, (loaded_ref, loaded_t_ref)))
    ]
    for copy in copies:
        copy.start()
    radix = total_rows // LANES
    chunks = LANES // width
    device = device_ref[0]
    tile, place = device // chunks, device % chunks
    lane = lax.broadcasted_iota(jnp.int32, (1, LANES), 1)
    col_class = jnp.where(tile == 0, 0, jnp.where(tile == 1, total_cols // LANES // 2, tile // 2))
    col_squares = wave_squares(col_class, place * width + lane % width, total_cols)
    col_scale = jnp.where(tile < 2, 1.0 / total_cols, 2.0 / total_cols).astype(jnp.float32)
    first = lane % HALF < width
    diffusion = jnp.where(first, SUBSTRATE_DIFFUSION, ACTIVATOR_DIFFUSION).astype(jnp.float32)
    decay = jnp.where(first, FEED_RATE, FEED_RATE + KILL_RATE).astype(jnp.float32)
    sign = jnp.where(first, -1.0, 1.0).astype(jnp.float32)
    k2 = lax.broadcasted_iota(jnp.int32, (LANES, LANES), 0)
    for index in range(radix // 2):
        for half in range(2):
            k1 = half * (radix // 2) if index == 0 else index
            scale = col_scale * ((1.0 if index == 0 else 2.0) / total_rows)
            linear = -diffusion * (wave_squares(k1, k2, total_rows) + col_squares) - decay
            growth = jnp.exp(linear * (0.5 * TIME_STEP))
            rows = slice(half * LANES, (half + 1) * LANES)
            forcing = (growth - 1.0) / linear * sign
            table_ref[index, rows, :] = jnp.where(lane < HALF, growth, forcing) * scale
    for copy in copies:
        copy.wait()


def forward_kernel(packed, place_ref, *refs):
    *block_refs, matrix_ref, out_ref, buffer_ref = refs
    count = len(block_refs)
    place = place_ref[0]
    for step, block_ref in zip(steps(count), block_refs):
        buffer_ref[place ^ step] = block_ref[...]
    cols = buffer_ref.shape[-1]
    height = buffer_ref.shape[2]
    tiles = []
    for source in range(count):
        for tile in range(cols // LANES):
            part = slice(tile * LANES, (tile + 1) * LANES)
            substrate = buffer_ref[source, 0, :, part]
            activator = buffer_ref[source, 1, :, part]
            tiles.append(jnp.concatenate([substrate, activator, substrate * activator * activator], axis=0))
    operands = paired(real_dft(tiles), 1)
    for index, operand in enumerate(operands):
        product = dot_pairs(split_value(operand), (matrix_ref[0, index], matrix_ref[1, index]))
        for half in range(2):
            tile = 2 * index + half
            spectrum = product[:, half * LANES : (half + 1) * LANES]
            if not packed:
                out_ref[tile] = spectrum
                continue
            for field in range(3):
                part = spectrum[field * height : (field + 1) * height]
                for chunk, piece in enumerate(swap_chunks([sublane_rows(part, group) for group in range(count)])):
                    out_ref[tile * count + chunk, field * SUBLANES : (field + 1) * SUBLANES, :] = piece


def place_of(band, source, bands):
    return (source * CORES + band % CORES) * (bands // CORES) + band // CORES


def advance_kernel(packed, count, in_ref, table_ref, matrix_ref, matrix_t_ref, out_ref):
    if packed:
        radix = in_ref.shape[0] // count
        tiles = []
        for band in range(radix):
            rows = []
            for source in range(count):
                block = in_ref[place_of(band, source, radix)]
                rows += swap_chunks([sublane_rows(block, min(field, 2)) for field in range(count)])
            tiles.append(jnp.concatenate(rows, axis=0))
    else:
        radix = in_ref.shape[0]
        tiles = [in_ref[band] for band in range(radix)]
    operands = paired(real_dft(tiles), 0)
    low_half = lax.broadcasted_iota(jnp.int32, (2 * LANES, LANES), 1) < HALF
    scaled = []
    for index, operand in enumerate(operands):
        high, low = split_value(operand)
        both = dot(matrix_t_ref[0, index], jnp.concatenate([high, low], axis=1))
        spectrum = both[:, :LANES] + (both[:, LANES:] + dot(matrix_t_ref[1, index], high))
        scaled.append(table_ref[index] * spectrum)
    products = []
    for index, value in enumerate(scaled):
        advanced = value + pltpu.roll(value, HALF, 1)
        high = advanced.astype(jnp.bfloat16).astype(jnp.float32)
        both = dot(matrix_ref[0, index], jnp.where(low_half, high, advanced - high).astype(jnp.bfloat16))
        rest = dot(matrix_ref[1, index], high.astype(jnp.bfloat16))
        products.append(both + (pltpu.roll(both, HALF, 1) + rest))
    bands = real_dft_transposed(unpaired(products, 0))
    low_half = lane_chunk((SUBLANES, LANES), HALF) == 0
    even = lane_chunk((SUBLANES, LANES), HALF // 2) % 2 == 0
    for band, value in enumerate(bands):
        if not packed:
            out_ref[band] = value
            continue
        for target in range(count):
            part = value[target * LANES // count : (target + 1) * LANES // count]
            near = jnp.where(low_half, sublane_rows(part, 0), sublane_rows(part, 2))
            far = jnp.where(low_half, sublane_rows(part, 1), sublane_rows(part, 3))
            place = place_of(band, target, radix)
            out_ref[place, :SUBLANES, :] = jnp.where(even, near, pltpu.roll(far, HALF // 2, 1))
            out_ref[place, SUBLANES:, :] = jnp.where(even, pltpu.roll(near, LANES - HALF // 2, 1), far)


def inverse_kernel(packed, count, shift, place_ref, in_ref, matrix_t_ref, *refs):
    place = place_ref[0]
    *out_refs, buffer_ref = refs
    radix = 2 * matrix_t_ref.shape[1]
    _, height, cols = out_refs[0].shape
    tiles = []
    for tile in range(radix):
        if not packed:
            tiles.append(in_ref[tile])
            continue
        rows = []
        for field in range(2):
            rows += swap_chunks([sublane_rows(in_ref[tile * count + chunk], field) for chunk in range(count)])
        tiles.append(jnp.concatenate(rows, axis=0))
    products = []
    for index in range(radix // 2):
        operand = jnp.concatenate([tiles[2 * index], tiles[2 * index + 1]], axis=1)
        products.append(dot_pairs(split_value(operand), (matrix_t_ref[0, index], matrix_t_ref[1, index])))
    values = real_dft_transposed(unpaired(products, 1))
    per_target = cols // LANES
    for index, value in enumerate(values):
        target, tile = index // per_target, index % per_target
        part = slice(tile * LANES, (tile + 1) * LANES)
        buffer_ref[place ^ target, 0, :, part] = value[:height] + shift
        buffer_ref[place ^ target, 1, :, part] = value[height:]
    for step, out_ref in zip(steps(count), out_refs):
        out_ref[...] = buffer_ref[step]


def steps(count):
    return [0, count - 1] + list(range(1, count - 1))


def start_all(copies):
    for copy in copies:
        copy.start()
    for copy in copies:
        copy.wait()


def cut_kernel(place_ref, *refs):
    *field_refs, semaphores = refs
    in_refs, out_refs = field_refs[:2], field_refs[2:]
    height = out_refs[0].shape[1]
    copies = []
    for index, (step, out_ref) in enumerate(zip(steps(len(out_refs)), out_refs)):
        rows = pl.ds((place_ref[0] ^ step) * height, height)
        for field, in_ref in enumerate(in_refs):
            copies.append(pltpu.make_async_copy(in_ref.at[rows], out_ref.at[field], semaphores.at[index, field]))
    start_all(copies)


def join_kernel(place_ref, *refs):
    *block_refs, first_ref, second_ref, semaphores = refs
    height = block_refs[0].shape[1]
    copies = []
    for index, (step, block_ref) in enumerate(zip(steps(len(block_refs)), block_refs)):
        rows = pl.ds((place_ref[0] ^ step) * height, height)
        for field, out_ref in enumerate((first_ref, second_ref)):
            copies.append(pltpu.make_async_copy(block_ref.at[field], out_ref.at[rows], semaphores.at[index, field]))
    start_all(copies)


def call(kernel, out_shape, specs, operands, scratch=(), out_spec=VMEM):
    return pl.pallas_call(
        kernel,
        out_shape=out_shape,
        in_specs=specs,
        out_specs=jax.tree.map(lambda _: out_spec, out_shape),
        scratch_shapes=list(scratch),
        compiler_params=pltpu.CompilerParams(vmem_limit_bytes=VMEM_LIMIT),
    )(*operands)


def in_hbm(value):
    return pltpu.with_memory_space_constraint(value, pltpu.HBM)


def float_shape(*shape):
    return jax.ShapeDtypeStruct(shape, jnp.float32)


def swap_blocks(blocks):
    count = len(blocks)
    return [blocks[0]] + [
        lax.ppermute(block, "col", [(s, s ^ step) for s in range(count)])
        for step, block in list(zip(steps(count), blocks))[1:]
    ]


def on_device(substrate, activator):
    row_count, col_count = substrate.shape
    bands, count = lax.axis_size("outer") * lax.axis_size("core"), lax.axis_size("col")
    total_rows, total_cols = row_count * bands, col_count * count
    height = row_count // count
    radix = total_cols // LANES
    width = total_cols // (bands * count)
    assert row_count == LANES and total_rows == total_cols and count & (count - 1) == 0
    packed = count == 4 and height == SUBLANES * count and width * count == LANES
    place = lax.axis_index("col")
    places = place[None].astype(jnp.int32)
    axes = ("col", "core", "outer")
    devices = lax.axis_index(axes)[None].astype(jnp.int32)
    matrices = basis_matrices(total_rows)
    forward = split_constant(matrices)
    backward = split_constant(np.swapaxes(matrices, 1, 2))

    block = float_shape(2, height, col_count)
    blocks = swap_blocks(
        call(
            cut_kernel,
            [block] * count,
            [SMEM] + [HBM] * 2,
            (places, in_hbm(substrate), in_hbm(activator)),
            [pltpu.SemaphoreType.DMA((count, 2))],
        )
    )
    table, forward, backward = call(
        lambda *refs: tables_kernel(total_rows, total_cols, width, *refs),
        [float_shape(radix // 2, 2 * LANES, LANES)]
        + [jax.ShapeDtypeStruct(constant.shape, constant.dtype) for constant in (forward, backward)],
        [SMEM, HBM, HBM],
        (devices, in_hbm(forward), in_hbm(backward)),
        [pltpu.SemaphoreType.DMA((2,))],
    )
    spectra = call(
        lambda *refs: forward_kernel(packed, *refs),
        float_shape(bands * count, 3 * SUBLANES, LANES) if packed else float_shape(radix, 3 * height, LANES),
        [SMEM] + [VMEM] * (count + 1),
        (places, *blocks, forward),
        [pltpu.VMEM((count, 2, height, col_count), jnp.float32)],
    )
    if packed:
        spectra = lax.all_to_all(spectra, axes, 0, 0, tiled=True)
    else:
        spectra = spectra.reshape(radix, 3, height, LANES // width, width)
        spectra = jnp.transpose(spectra, (0, 3, 1, 2, 4)).reshape(bands * count, -1)
        spectra = lax.all_to_all(spectra, axes, 0, 0, tiled=True)
        spectra = spectra.reshape(count, CORES, bands // CORES, 3, height, width)
        spectra = jnp.transpose(spectra, (3, 2, 1, 0, 4, 5))
        spectra = spectra.reshape(3, bands, row_count, width)
        rest = jnp.zeros((bands, row_count, HALF - 2 * width), jnp.float32)
        spectra = jnp.concatenate([spectra[0], spectra[1], rest, spectra[2], spectra[2], rest], axis=2)
    advanced = call(
        lambda *refs: advance_kernel(packed, count, *refs),
        float_shape(bands * count, 2 * SUBLANES, LANES) if packed else float_shape(bands, row_count, LANES),
        [VMEM] * 4,
        (spectra, table, forward, backward),
    )
    if packed:
        advanced = lax.all_to_all(advanced, axes, 0, 0, tiled=True)
    else:
        advanced = advanced[:, :, : 2 * width].reshape(bands // CORES, CORES, count, height, 2, width)
        advanced = jnp.transpose(advanced, (2, 1, 0, 4, 3, 5)).reshape(bands * count, -1)
        advanced = lax.all_to_all(advanced, axes, 0, 0, tiled=True)
        advanced = jnp.transpose(advanced.reshape(radix, LANES // width, 2, height, width), (0, 2, 3, 1, 4))
        advanced = advanced.reshape(radix, 2 * height, LANES)
    shift = FEED_RATE * math.expm1(-FEED_RATE * 0.5 * TIME_STEP) / -FEED_RATE
    blocks = swap_blocks(
        call(
            lambda *refs: inverse_kernel(packed, count, shift, *refs),
            [block] * count,
            [SMEM] + [VMEM] * 2,
            (places, advanced, backward),
            [pltpu.VMEM((count, 2, height, col_count), jnp.float32)],
        )
    )
    return tuple(
        call(
            join_kernel,
            [float_shape(row_count, col_count)] * 2,
            [SMEM] + [VMEM] * count,
            (places, *blocks),
            [pltpu.SemaphoreType.DMA((count, 2))],
            HBM,
        )
    )


def solution(mesh):
    bands, count = mesh.shape["row"], mesh.shape["col"]
    split = Mesh(mesh.devices.reshape(bands // CORES, CORES, count), ("outer", "core", "col"))
    spec = P(("outer", "core"), "col")
    return jax.shard_map(on_device, mesh=split, in_specs=(spec, spec), out_specs=(spec, spec), check_vma=False)
```

```python
import math

import jax
import jax.numpy as jnp
import numpy as np
from jax import lax
from jax.experimental import pallas as pl
from jax.experimental.pallas import tpu as pltpu
from jax.sharding import Mesh
from jax.sharding import PartitionSpec as P

FEED_RATE = 0.037
KILL_RATE = 0.06
TIME_STEP = 8.0
SUBSTRATE_DIFFUSION = 4e-07
ACTIVATOR_DIFFUSION = 2e-07
LANES = 128
HALF = LANES // 2
CORES = 2
PAIR = 2
COL = ("col_high", "col_low")
SUBLANES = 8
VMEM_LIMIT = 36 << 20
VMEM = pl.BlockSpec(memory_space=pltpu.VMEM)
HBM = pl.BlockSpec(memory_space=pltpu.HBM)
SMEM = pl.BlockSpec(memory_space=pltpu.SMEM)


def basis_matrices(total):
    radix = total // LANES
    b = np.arange(LANES, dtype=np.int64)[:, None]
    k2 = np.arange(LANES, dtype=np.int64)[None, :]

    def angles(k1):
        return (b * (k1 + radix * k2) % total) * (2.0 * np.pi / total)

    matrices = np.zeros((radix // 2, 2 * LANES, 2 * LANES))
    for half, k1 in enumerate((0, radix // 2)):
        theta = angles(k1)
        part = slice(half * LANES, (half + 1) * LANES)
        matrices[0, part, part] = np.cos(theta) + np.sin(theta)
    for k1 in range(1, radix // 2):
        cosine, sine = np.cos(angles(k1)), np.sin(angles(k1))
        matrices[k1] = np.block([[cosine, -sine], [sine, cosine]])
    return matrices


def split_constant(matrices):
    high = matrices.astype(jnp.bfloat16)
    low = (matrices - high.astype(np.float64)).astype(jnp.bfloat16)
    return jnp.asarray(np.stack([high, low]))


def split_value(values):
    high = values.astype(jnp.bfloat16)
    low = (values - high.astype(jnp.float32)).astype(jnp.bfloat16)
    return high, low


def dot(left, right):
    return jnp.dot(left, right, preferred_element_type=jnp.float32)


def dot_pairs(left, right):
    height = left[0].shape[0]
    both = dot(jnp.concatenate(left, axis=0), right[0])
    return both[:height] + (both[height:] + dot(left[0], right[1]))


def turn(value, k, period, sign):
    real, imag = value
    if k == 0:
        return value
    if 4 * k == period:
        return (-sign * imag, sign * real) if imag is not None else (None, sign * real)
    cosine, sine = math.cos(2.0 * math.pi * k / period), sign * math.sin(2.0 * math.pi * k / period)
    if imag is None:
        return (real * cosine, real * sine)
    if 8 * k == period:
        return ((real - sign * imag) * cosine, (imag + sign * real) * cosine)
    return (real * cosine - imag * sine, real * sine + imag * cosine)


def plus(left, right):
    if left is None or right is None:
        return left if right is None else right
    return left + right


def minus(left, right):
    if right is None:
        return left
    return -right if left is None else left - right


def real_dft(values):
    n = len(values)
    if n == 1:
        return [(values[0], None)]
    even, odd = real_dft(values[0::2]), real_dft(values[1::2])
    out = [None] * (n // 2 + 1)
    for k in range(n // 4 + 1):
        turned = turn(odd[k], k, n, -1.0)
        if n // 2 - k != k:
            out[n // 2 - k] = (minus(even[k][0], turned[0]), minus(turned[1], even[k][1]))
        out[k] = (plus(even[k][0], turned[0]), plus(even[k][1], turned[1]))
    return out


def real_dft_transposed(spectrum):
    n = 2 * (len(spectrum) - 1)
    if n == 0:
        return [spectrum[0][0]]
    even, odd = [], []
    for k in range(n // 4 + 1):
        near, far = spectrum[k], spectrum[n // 2 - k]
        if k == 0:
            even.append((near[0] + far[0], None))
            odd.append((near[0] - far[0], None))
        elif 4 * k == n:
            even.append((near[0], None))
            odd.append((-near[1], None))
        else:
            even.append((near[0] + far[0], near[1] - far[1]))
            odd.append(turn((near[0] - far[0], near[1] + far[1]), k, n, 1.0))
    out = [None] * n
    out[0::2] = real_dft_transposed(even)
    out[1::2] = real_dft_transposed(odd)
    return out


def paired(spectrum, axis):
    half = len(spectrum) - 1
    rows = [(spectrum[0][0], spectrum[half][0])] + spectrum[1:half]
    return [jnp.concatenate(row, axis=axis) for row in rows]


def unpaired(products, axis):
    def halves(value):
        return lax.slice_in_dim(value, 0, LANES, axis=axis), lax.slice_in_dim(value, LANES, 2 * LANES, axis=axis)

    parts = [halves(value) for value in products]
    first, last = parts[0]
    return [(first, None)] + parts[1:] + [(last, None)]


def lane_chunk(shape, width):
    return lax.broadcasted_iota(jnp.int32, shape, len(shape) - 1) // width


def swap_chunks(pieces):
    pieces = list(pieces)
    count = len(pieces)
    width = LANES // count
    chunk = lane_chunk(pieces[0].shape, width)
    step = count // 2
    while step:
        stays = chunk & step == 0
        for first in range(count):
            if first & step:
                continue
            near, far = pieces[first], pieces[first + step]
            pieces[first] = jnp.where(stays, near, pltpu.roll(far, step * width, 1))
            pieces[first + step] = jnp.where(stays, pltpu.roll(near, LANES - step * width, 1), far)
        step //= 2
    return pieces


def sublane_rows(value, group):
    return value[group * SUBLANES : (group + 1) * SUBLANES]


def wave_squares(k1, k2, total):
    radix = total // LANES
    wave = k1 + radix * k2
    signed = jnp.where(2 * wave < total, wave, wave - total).astype(jnp.float32)
    angular = (2.0 * math.pi) * signed
    return angular * angular


def tables_kernel(total_rows, total_cols, width, device_ref, *refs):
    *matrix_refs, table_ref, loaded_ref, loaded_t_ref, semaphores = refs
    copies = [
        pltpu.make_async_copy(source, target, semaphores.at[index])
        for index, (source, target) in enumerate(zip(matrix_refs, (loaded_ref, loaded_t_ref)))
    ]
    for copy in copies:
        copy.start()
    radix = total_rows // LANES
    chunks = LANES // width
    device = device_ref[0]
    tile, place = device // chunks, device % chunks
    lane = lax.broadcasted_iota(jnp.int32, (1, LANES), 1)
    col_class = jnp.where(tile == 0, 0, jnp.where(tile == 1, total_cols // LANES // 2, tile // 2))
    col_squares = wave_squares(col_class, place * width + lane % width, total_cols)
    col_scale = jnp.where(tile < 2, 1.0 / total_cols, 2.0 / total_cols).astype(jnp.float32)
    first = lane % HALF < width
    diffusion = jnp.where(first, SUBSTRATE_DIFFUSION, ACTIVATOR_DIFFUSION).astype(jnp.float32)
    decay = jnp.where(first, FEED_RATE, FEED_RATE + KILL_RATE).astype(jnp.float32)
    sign = jnp.where(first, -1.0, 1.0).astype(jnp.float32)
    k2 = lax.broadcasted_iota(jnp.int32, (LANES, LANES), 0)
    for index in range(radix // 2):
        for half in range(2):
            k1 = half * (radix // 2) if index == 0 else index
            scale = col_scale * ((1.0 if index == 0 else 2.0) / total_rows)
            linear = -diffusion * (wave_squares(k1, k2, total_rows) + col_squares) - decay
            growth = jnp.exp(linear * (0.5 * TIME_STEP))
            rows = slice(half * LANES, (half + 1) * LANES)
            forcing = (growth - 1.0) / linear * sign
            table_ref[index, rows, :] = jnp.where(lane < HALF, growth, forcing) * scale
    for copy in copies:
        copy.wait()


def forward_kernel(packed, place_ref, *refs):
    *block_refs, matrix_ref, out_ref, buffer_ref = refs
    count = len(block_refs)
    place = place_ref[0]
    for step, block_ref in zip(steps(count), block_refs):
        buffer_ref[place ^ step] = block_ref[...]
    cols = buffer_ref.shape[-1]
    height = buffer_ref.shape[2]
    tiles = []
    for source in range(count):
        for tile in range(cols // LANES):
            part = slice(tile * LANES, (tile + 1) * LANES)
            substrate = buffer_ref[source, 0, :, part]
            activator = buffer_ref[source, 1, :, part]
            tiles.append(jnp.concatenate([substrate, activator, substrate * activator * activator], axis=0))
    operands = paired(real_dft(tiles), 1)
    for index, operand in enumerate(operands):
        product = dot_pairs(split_value(operand), (matrix_ref[0, index], matrix_ref[1, index]))
        for half in range(2):
            tile = 2 * index + half
            spectrum = product[:, half * LANES : (half + 1) * LANES]
            if not packed:
                out_ref[tile] = spectrum
                continue
            for field in range(3):
                part = spectrum[field * height : (field + 1) * height]
                for chunk, piece in enumerate(swap_chunks([sublane_rows(part, group) for group in range(count)])):
                    out_ref[tile * count + chunk, field * SUBLANES : (field + 1) * SUBLANES, :] = piece


def place_of(band, source, bands):
    outer, core = band // CORES, band % CORES
    high, low = source // PAIR, source % PAIR
    return ((high * CORES + core) * PAIR + low) * (bands // CORES) + outer


def advance_kernel(packed, count, in_ref, table_ref, matrix_ref, matrix_t_ref, out_ref):
    if packed:
        radix = in_ref.shape[0] // count
        tiles = []
        for band in range(radix):
            rows = []
            for source in range(count):
                block = in_ref[place_of(band, source, radix)]
                rows += swap_chunks([sublane_rows(block, min(field, 2)) for field in range(count)])
            tiles.append(jnp.concatenate(rows, axis=0))
    else:
        radix = in_ref.shape[0]
        tiles = [in_ref[band] for band in range(radix)]
    operands = paired(real_dft(tiles), 0)
    low_half = lax.broadcasted_iota(jnp.int32, (2 * LANES, LANES), 1) < HALF
    scaled = []
    for index, operand in enumerate(operands):
        high, low = split_value(operand)
        both = dot(matrix_t_ref[0, index], jnp.concatenate([high, low], axis=1))
        spectrum = both[:, :LANES] + (both[:, LANES:] + dot(matrix_t_ref[1, index], high))
        scaled.append(table_ref[index] * spectrum)
    products = []
    for index, value in enumerate(scaled):
        advanced = value + pltpu.roll(value, HALF, 1)
        high = advanced.astype(jnp.bfloat16).astype(jnp.float32)
        both = dot(matrix_ref[0, index], jnp.where(low_half, high, advanced - high).astype(jnp.bfloat16))
        rest = dot(matrix_ref[1, index], high.astype(jnp.bfloat16))
        products.append(both + (pltpu.roll(both, HALF, 1) + rest))
    bands = real_dft_transposed(unpaired(products, 0))
    low_half = lane_chunk((SUBLANES, LANES), HALF) == 0
    even = lane_chunk((SUBLANES, LANES), HALF // 2) % 2 == 0
    for band, value in enumerate(bands):
        if not packed:
            out_ref[band] = value
            continue
        for target in range(count):
            part = value[target * LANES // count : (target + 1) * LANES // count]
            near = jnp.where(low_half, sublane_rows(part, 0), sublane_rows(part, 2))
            far = jnp.where(low_half, sublane_rows(part, 1), sublane_rows(part, 3))
            place = place_of(band, target, radix)
            out_ref[place, :SUBLANES, :] = jnp.where(even, near, pltpu.roll(far, HALF // 2, 1))
            out_ref[place, SUBLANES:, :] = jnp.where(even, pltpu.roll(near, LANES - HALF // 2, 1), far)


def inverse_kernel(packed, count, shift, place_ref, in_ref, matrix_t_ref, *refs):
    place = place_ref[0]
    *out_refs, buffer_ref = refs
    radix = 2 * matrix_t_ref.shape[1]
    _, height, cols = out_refs[0].shape
    tiles = []
    for tile in range(radix):
        if not packed:
            tiles.append(in_ref[tile])
            continue
        rows = []
        for field in range(2):
            rows += swap_chunks([sublane_rows(in_ref[tile * count + chunk], field) for chunk in range(count)])
        tiles.append(jnp.concatenate(rows, axis=0))
    products = []
    for index in range(radix // 2):
        operand = jnp.concatenate([tiles[2 * index], tiles[2 * index + 1]], axis=1)
        products.append(dot_pairs(split_value(operand), (matrix_t_ref[0, index], matrix_t_ref[1, index])))
    values = real_dft_transposed(unpaired(products, 1))
    per_target = cols // LANES
    for index, value in enumerate(values):
        target, tile = index // per_target, index % per_target
        part = slice(tile * LANES, (tile + 1) * LANES)
        buffer_ref[place ^ target, 0, :, part] = value[:height] + shift
        buffer_ref[place ^ target, 1, :, part] = value[height:]
    for step, out_ref in zip(steps(count), out_refs):
        out_ref[...] = buffer_ref[step]


def steps(count):
    return [0, count - 1] + list(range(1, count - 1))


def start_all(copies):
    for copy in copies:
        copy.start()
    for copy in copies:
        copy.wait()


def cut_kernel(place_ref, *refs):
    *field_refs, semaphores = refs
    in_refs, out_refs = field_refs[:2], field_refs[2:]
    height = out_refs[0].shape[1]
    copies = []
    for index, (step, out_ref) in enumerate(zip(steps(len(out_refs)), out_refs)):
        rows = pl.ds((place_ref[0] ^ step) * height, height)
        for field, in_ref in enumerate(in_refs):
            copies.append(pltpu.make_async_copy(in_ref.at[rows], out_ref.at[field], semaphores.at[index, field]))
    start_all(copies)


def join_kernel(place_ref, *refs):
    *block_refs, first_ref, second_ref, semaphores = refs
    height = block_refs[0].shape[1]
    copies = []
    for index, (step, block_ref) in enumerate(zip(steps(len(block_refs)), block_refs)):
        rows = pl.ds((place_ref[0] ^ step) * height, height)
        for field, out_ref in enumerate((first_ref, second_ref)):
            copies.append(pltpu.make_async_copy(block_ref.at[field], out_ref.at[rows], semaphores.at[index, field]))
    start_all(copies)


def call(kernel, out_shape, specs, operands, scratch=(), out_spec=VMEM):
    return pl.pallas_call(
        kernel,
        out_shape=out_shape,
        in_specs=specs,
        out_specs=jax.tree.map(lambda _: out_spec, out_shape),
        scratch_shapes=list(scratch),
        compiler_params=pltpu.CompilerParams(vmem_limit_bytes=VMEM_LIMIT),
    )(*operands)


def in_hbm(value):
    return pltpu.with_memory_space_constraint(value, pltpu.HBM)


def float_shape(*shape):
    return jax.ShapeDtypeStruct(shape, jnp.float32)


def swap_blocks(blocks):
    count = len(blocks)
    return [blocks[0]] + [
        lax.ppermute(block, COL, [(s, s ^ step) for s in range(count)])
        for step, block in list(zip(steps(count), blocks))[1:]
    ]


def on_device(substrate, activator):
    row_count, col_count = substrate.shape
    bands, count = lax.axis_size("outer") * lax.axis_size("core"), lax.axis_size(COL)
    total_rows, total_cols = row_count * bands, col_count * count
    height = row_count // count
    radix = total_cols // LANES
    width = total_cols // (bands * count)
    assert row_count == LANES and total_rows == total_cols and count & (count - 1) == 0
    packed = count == 4 and height == SUBLANES * count and width * count == LANES
    place = lax.axis_index(COL)
    places = place[None].astype(jnp.int32)
    axes = ("col_high", "core", "col_low", "outer")
    devices = lax.axis_index(axes)[None].astype(jnp.int32)
    matrices = basis_matrices(total_rows)
    forward = split_constant(matrices)
    backward = split_constant(np.swapaxes(matrices, 1, 2))

    block = float_shape(2, height, col_count)
    blocks = swap_blocks(
        call(
            cut_kernel,
            [block] * count,
            [SMEM] + [HBM] * 2,
            (places, in_hbm(substrate), in_hbm(activator)),
            [pltpu.SemaphoreType.DMA((count, 2))],
        )
    )
    table, forward, backward = call(
        lambda *refs: tables_kernel(total_rows, total_cols, width, *refs),
        [float_shape(radix // 2, 2 * LANES, LANES)]
        + [jax.ShapeDtypeStruct(constant.shape, constant.dtype) for constant in (forward, backward)],
        [SMEM, HBM, HBM],
        (devices, in_hbm(forward), in_hbm(backward)),
        [pltpu.SemaphoreType.DMA((2,))],
    )
    spectra = call(
        lambda *refs: forward_kernel(packed, *refs),
        float_shape(bands * count, 3 * SUBLANES, LANES) if packed else float_shape(radix, 3 * height, LANES),
        [SMEM] + [VMEM] * (count + 1),
        (places, *blocks, forward),
        [pltpu.VMEM((count, 2, height, col_count), jnp.float32)],
    )
    if packed:
        spectra = lax.all_to_all(spectra, axes, 0, 0, tiled=True)
    else:
        spectra = spectra.reshape(radix, 3, height, LANES // width, width)
        spectra = jnp.transpose(spectra, (0, 3, 1, 2, 4)).reshape(bands * count, -1)
        spectra = lax.all_to_all(spectra, axes, 0, 0, tiled=True)
        spectra = spectra.reshape(count // PAIR, CORES, PAIR, bands // CORES, 3, height, width)
        spectra = jnp.transpose(spectra, (4, 3, 1, 0, 2, 5, 6))
        spectra = spectra.reshape(3, bands, row_count, width)
        rest = jnp.zeros((bands, row_count, HALF - 2 * width), jnp.float32)
        spectra = jnp.concatenate([spectra[0], spectra[1], rest, spectra[2], spectra[2], rest], axis=2)
    advanced = call(
        lambda *refs: advance_kernel(packed, count, *refs),
        float_shape(bands * count, 2 * SUBLANES, LANES) if packed else float_shape(bands, row_count, LANES),
        [VMEM] * 4,
        (spectra, table, forward, backward),
    )
    if packed:
        advanced = lax.all_to_all(advanced, axes, 0, 0, tiled=True)
    else:
        advanced = advanced[:, :, : 2 * width].reshape(bands // CORES, CORES, count // PAIR, PAIR, height, 2, width)
        advanced = jnp.transpose(advanced, (2, 1, 3, 0, 5, 4, 6)).reshape(bands * count, -1)
        advanced = lax.all_to_all(advanced, axes, 0, 0, tiled=True)
        advanced = jnp.transpose(advanced.reshape(radix, LANES // width, 2, height, width), (0, 2, 3, 1, 4))
        advanced = advanced.reshape(radix, 2 * height, LANES)
    shift = FEED_RATE * math.expm1(-FEED_RATE * 0.5 * TIME_STEP) / -FEED_RATE
    blocks = swap_blocks(
        call(
            lambda *refs: inverse_kernel(packed, count, shift, *refs),
            [block] * count,
            [SMEM] + [VMEM] * 2,
            (places, advanced, backward),
            [pltpu.VMEM((count, 2, height, col_count), jnp.float32)],
        )
    )
    return tuple(
        call(
            join_kernel,
            [float_shape(row_count, col_count)] * 2,
            [SMEM] + [VMEM] * count,
            (places, *blocks),
            [pltpu.SemaphoreType.DMA((count, 2))],
            HBM,
        )
    )


def solution(mesh):
    bands, count = mesh.shape["row"], mesh.shape["col"]
    split = Mesh(mesh.devices.reshape(bands // CORES, CORES, count // PAIR, PAIR), ("outer", "core") + COL)
    spec = P(("outer", "core"), COL)
    return jax.shard_map(on_device, mesh=split, in_specs=(spec, spec), out_specs=(spec, spec), check_vma=False)
```

```python
import math

import jax
import jax.numpy as jnp
import numpy as np
from jax import lax
from jax.experimental import pallas as pl
from jax.experimental.pallas import tpu as pltpu
from jax.sharding import Mesh
from jax.sharding import PartitionSpec as P

FEED_RATE = 0.037
KILL_RATE = 0.06
TIME_STEP = 8.0
SUBSTRATE_DIFFUSION = 4e-07
ACTIVATOR_DIFFUSION = 2e-07
LANES = 128
HALF = LANES // 2
CORES = 2
AXES = ("col", "core", "outer")
SUBLANES = 8
VMEM_LIMIT = 36 << 20
VMEM = pl.BlockSpec(memory_space=pltpu.VMEM)
HBM = pl.BlockSpec(memory_space=pltpu.HBM)


def basis_matrices(total):
    radix = total // LANES
    b = np.arange(LANES, dtype=np.int64)[:, None]
    k2 = np.arange(LANES, dtype=np.int64)[None, :]

    def angles(k1):
        return (b * (k1 + radix * k2) % total) * (2.0 * np.pi / total)

    matrices = np.zeros((radix // 2, 2 * LANES, 2 * LANES))
    for half, k1 in enumerate((0, radix // 2)):
        theta = angles(k1)
        part = slice(half * LANES, (half + 1) * LANES)
        matrices[0, part, part] = np.cos(theta) + np.sin(theta)
    for k1 in range(1, radix // 2):
        cosine, sine = np.cos(angles(k1)), np.sin(angles(k1))
        matrices[k1] = np.block([[cosine, -sine], [sine, cosine]])
    return matrices


def split_constant(matrices):
    high = matrices.astype(jnp.bfloat16)
    low = (matrices - high.astype(np.float64)).astype(jnp.bfloat16)
    return jnp.asarray(np.stack([high, low]))


def split_value(values):
    high = values.astype(jnp.bfloat16)
    low = (values - high.astype(jnp.float32)).astype(jnp.bfloat16)
    return high, low


def dot(left, right):
    return jnp.dot(left, right, preferred_element_type=jnp.float32)


def dot_pairs(left, right):
    height = left[0].shape[0]
    both = dot(jnp.concatenate(left, axis=0), right[0])
    return both[:height] + (both[height:] + dot(left[0], right[1]))


def turn(value, k, period, sign):
    real, imag = value
    if k == 0:
        return value
    if 4 * k == period:
        return (-sign * imag, sign * real) if imag is not None else (None, sign * real)
    cosine, sine = math.cos(2.0 * math.pi * k / period), sign * math.sin(2.0 * math.pi * k / period)
    if imag is None:
        return (real * cosine, real * sine)
    if 8 * k == period:
        return ((real - sign * imag) * cosine, (imag + sign * real) * cosine)
    return (real * cosine - imag * sine, real * sine + imag * cosine)


def plus(left, right):
    if left is None or right is None:
        return left if right is None else right
    return left + right


def minus(left, right):
    if right is None:
        return left
    return -right if left is None else left - right


def real_dft(values):
    n = len(values)
    if n == 1:
        return [(values[0], None)]
    even, odd = real_dft(values[0::2]), real_dft(values[1::2])
    out = [None] * (n // 2 + 1)
    for k in range(n // 4 + 1):
        turned = turn(odd[k], k, n, -1.0)
        if n // 2 - k != k:
            out[n // 2 - k] = (minus(even[k][0], turned[0]), minus(turned[1], even[k][1]))
        out[k] = (plus(even[k][0], turned[0]), plus(even[k][1], turned[1]))
    return out


def real_dft_transposed(spectrum):
    n = 2 * (len(spectrum) - 1)
    if n == 0:
        return [spectrum[0][0]]
    even, odd = [], []
    for k in range(n // 4 + 1):
        near, far = spectrum[k], spectrum[n // 2 - k]
        if k == 0:
            even.append((near[0] + far[0], None))
            odd.append((near[0] - far[0], None))
        elif 4 * k == n:
            even.append((near[0], None))
            odd.append((-near[1], None))
        else:
            even.append((near[0] + far[0], near[1] - far[1]))
            odd.append(turn((near[0] - far[0], near[1] + far[1]), k, n, 1.0))
    out = [None] * n
    out[0::2] = real_dft_transposed(even)
    out[1::2] = real_dft_transposed(odd)
    return out


def paired(spectrum, axis):
    half = len(spectrum) - 1
    rows = [(spectrum[0][0], spectrum[half][0])] + spectrum[1:half]
    return [jnp.concatenate(row, axis=axis) for row in rows]


def unpaired(products, axis):
    def halves(value):
        return lax.slice_in_dim(value, 0, LANES, axis=axis), lax.slice_in_dim(value, LANES, 2 * LANES, axis=axis)

    parts = [halves(value) for value in products]
    first, last = parts[0]
    return [(first, None)] + parts[1:] + [(last, None)]


def lane_chunk(shape, width):
    return lax.broadcasted_iota(jnp.int32, shape, len(shape) - 1) // width


def swap_chunks(pieces):
    pieces = list(pieces)
    count = len(pieces)
    width = LANES // count
    chunk = lane_chunk(pieces[0].shape, width)
    step = count // 2
    while step:
        stays = chunk & step == 0
        for first in range(count):
            if first & step:
                continue
            near, far = pieces[first], pieces[first + step]
            pieces[first] = jnp.where(stays, near, pltpu.roll(far, step * width, 1))
            pieces[first + step] = jnp.where(stays, pltpu.roll(near, LANES - step * width, 1), far)
        step //= 2
    return pieces


def sublane_rows(value, group):
    return value[group * SUBLANES : (group + 1) * SUBLANES]


def wave_squares(k1, k2, total):
    radix = total // LANES
    wave = k1 + radix * k2
    signed = jnp.where(2 * wave < total, wave, wave - total).astype(jnp.float32)
    angular = (2.0 * math.pi) * signed
    return angular * angular


def tables_kernel(total_rows, total_cols, width, *refs):
    *matrix_refs, table_ref, loaded_ref, loaded_t_ref, semaphores = refs
    copies = [
        pltpu.make_async_copy(source, target, semaphores.at[index])
        for index, (source, target) in enumerate(zip(matrix_refs, (loaded_ref, loaded_t_ref)))
    ]
    for copy in copies:
        copy.start()
    radix = total_rows // LANES
    chunks = LANES // width
    device = lax.axis_index(AXES)
    tile, place = device // chunks, device % chunks
    lane = lax.broadcasted_iota(jnp.int32, (1, LANES), 1)
    col_class = jnp.where(tile == 0, 0, jnp.where(tile == 1, total_cols // LANES // 2, tile // 2))
    col_squares = wave_squares(col_class, place * width + lane % width, total_cols)
    col_scale = jnp.where(tile < 2, 1.0 / total_cols, 2.0 / total_cols).astype(jnp.float32)
    first = lane % HALF < width
    diffusion = jnp.where(first, SUBSTRATE_DIFFUSION, ACTIVATOR_DIFFUSION).astype(jnp.float32)
    decay = jnp.where(first, FEED_RATE, FEED_RATE + KILL_RATE).astype(jnp.float32)
    sign = jnp.where(first, -1.0, 1.0).astype(jnp.float32)
    k2 = lax.broadcasted_iota(jnp.int32, (LANES, LANES), 0)
    for index in range(radix // 2):
        for half in range(2):
            k1 = half * (radix // 2) if index == 0 else index
            scale = col_scale * ((1.0 if index == 0 else 2.0) / total_rows)
            linear = -diffusion * (wave_squares(k1, k2, total_rows) + col_squares) - decay
            growth = jnp.exp(linear * (0.5 * TIME_STEP))
            rows = slice(half * LANES, (half + 1) * LANES)
            forcing = (growth - 1.0) / linear * sign
            table_ref[index, rows, :] = jnp.where(lane < HALF, growth, forcing) * scale
    for copy in copies:
        copy.wait()


def forward_kernel(packed, *refs):
    *block_refs, matrix_ref, out_ref, buffer_ref = refs
    count = len(block_refs)
    place = lax.axis_index("col")
    for step, block_ref in zip(steps(count), block_refs):
        buffer_ref[place ^ step] = block_ref[...]
    cols = buffer_ref.shape[-1]
    height = buffer_ref.shape[2]
    tiles = []
    for source in range(count):
        for tile in range(cols // LANES):
            part = slice(tile * LANES, (tile + 1) * LANES)
            substrate = buffer_ref[source, 0, :, part]
            activator = buffer_ref[source, 1, :, part]
            tiles.append(jnp.concatenate([substrate, activator, substrate * activator * activator], axis=0))
    operands = paired(real_dft(tiles), 1)
    for index, operand in enumerate(operands):
        product = dot_pairs(split_value(operand), (matrix_ref[0, index], matrix_ref[1, index]))
        for half in range(2):
            tile = 2 * index + half
            spectrum = product[:, half * LANES : (half + 1) * LANES]
            if not packed:
                out_ref[tile] = spectrum
                continue
            for field in range(3):
                part = spectrum[field * height : (field + 1) * height]
                for chunk, piece in enumerate(swap_chunks([sublane_rows(part, group) for group in range(count)])):
                    out_ref[tile * count + chunk, field * SUBLANES : (field + 1) * SUBLANES, :] = piece


def place_of(band, source, bands):
    return (source * CORES + band % CORES) * (bands // CORES) + band // CORES


def advance_kernel(packed, count, in_ref, table_ref, matrix_ref, matrix_t_ref, out_ref):
    if packed:
        radix = in_ref.shape[0] // count
        tiles = []
        for band in range(radix):
            rows = []
            for source in range(count):
                block = in_ref[place_of(band, source, radix)]
                rows += swap_chunks([sublane_rows(block, min(field, 2)) for field in range(count)])
            tiles.append(jnp.concatenate(rows, axis=0))
    else:
        radix = in_ref.shape[0]
        tiles = [in_ref[band] for band in range(radix)]
    operands = paired(real_dft(tiles), 0)
    low_half = lax.broadcasted_iota(jnp.int32, (2 * LANES, LANES), 1) < HALF
    scaled = []
    for index, operand in enumerate(operands):
        high, low = split_value(operand)
        both = dot(matrix_t_ref[0, index], jnp.concatenate([high, low], axis=1))
        spectrum = both[:, :LANES] + (both[:, LANES:] + dot(matrix_t_ref[1, index], high))
        scaled.append(table_ref[index] * spectrum)
    products = []
    for index, value in enumerate(scaled):
        advanced = value + pltpu.roll(value, HALF, 1)
        high = advanced.astype(jnp.bfloat16).astype(jnp.float32)
        both = dot(matrix_ref[0, index], jnp.where(low_half, high, advanced - high).astype(jnp.bfloat16))
        rest = dot(matrix_ref[1, index], high.astype(jnp.bfloat16))
        products.append(both + (pltpu.roll(both, HALF, 1) + rest))
    bands = real_dft_transposed(unpaired(products, 0))
    low_half = lane_chunk((SUBLANES, LANES), HALF) == 0
    even = lane_chunk((SUBLANES, LANES), HALF // 2) % 2 == 0
    for band, value in enumerate(bands):
        if not packed:
            out_ref[band] = value
            continue
        for target in range(count):
            part = value[target * LANES // count : (target + 1) * LANES // count]
            near = jnp.where(low_half, sublane_rows(part, 0), sublane_rows(part, 2))
            far = jnp.where(low_half, sublane_rows(part, 1), sublane_rows(part, 3))
            place = place_of(band, target, radix)
            out_ref[place, :SUBLANES, :] = jnp.where(even, near, pltpu.roll(far, HALF // 2, 1))
            out_ref[place, SUBLANES:, :] = jnp.where(even, pltpu.roll(near, LANES - HALF // 2, 1), far)


def inverse_kernel(packed, count, shift, in_ref, matrix_t_ref, *refs):
    place = lax.axis_index("col")
    *out_refs, buffer_ref = refs
    radix = 2 * matrix_t_ref.shape[1]
    _, height, cols = out_refs[0].shape
    tiles = []
    for tile in range(radix):
        if not packed:
            tiles.append(in_ref[tile])
            continue
        rows = []
        for field in range(2):
            rows += swap_chunks([sublane_rows(in_ref[tile * count + chunk], field) for chunk in range(count)])
        tiles.append(jnp.concatenate(rows, axis=0))
    products = []
    for index in range(radix // 2):
        operand = jnp.concatenate([tiles[2 * index], tiles[2 * index + 1]], axis=1)
        products.append(dot_pairs(split_value(operand), (matrix_t_ref[0, index], matrix_t_ref[1, index])))
    values = real_dft_transposed(unpaired(products, 1))
    per_target = cols // LANES
    for index, value in enumerate(values):
        target, tile = index // per_target, index % per_target
        part = slice(tile * LANES, (tile + 1) * LANES)
        buffer_ref[place ^ target, 0, :, part] = value[:height] + shift
        buffer_ref[place ^ target, 1, :, part] = value[height:]
    for step, out_ref in zip(steps(count), out_refs):
        out_ref[...] = buffer_ref[step]


def steps(count):
    return [0, count - 1] + list(range(1, count - 1))


def start_all(copies):
    for copy in copies:
        copy.start()
    for copy in copies:
        copy.wait()


def cut_kernel(*refs):
    *field_refs, semaphores = refs
    in_refs, out_refs = field_refs[:2], field_refs[2:]
    height = out_refs[0].shape[1]
    copies = []
    for index, (step, out_ref) in enumerate(zip(steps(len(out_refs)), out_refs)):
        rows = pl.ds((lax.axis_index("col") ^ step) * height, height)
        for field, in_ref in enumerate(in_refs):
            copies.append(pltpu.make_async_copy(in_ref.at[rows], out_ref.at[field], semaphores.at[index, field]))
    start_all(copies)


def join_kernel(*refs):
    *block_refs, first_ref, second_ref, semaphores = refs
    height = block_refs[0].shape[1]
    copies = []
    for index, (step, block_ref) in enumerate(zip(steps(len(block_refs)), block_refs)):
        rows = pl.ds((lax.axis_index("col") ^ step) * height, height)
        for field, out_ref in enumerate((first_ref, second_ref)):
            copies.append(pltpu.make_async_copy(block_ref.at[field], out_ref.at[rows], semaphores.at[index, field]))
    start_all(copies)


def call(kernel, out_shape, specs, operands, scratch=(), out_spec=VMEM):
    return pl.pallas_call(
        kernel,
        out_shape=out_shape,
        in_specs=specs,
        out_specs=jax.tree.map(lambda _: out_spec, out_shape),
        scratch_shapes=list(scratch),
        compiler_params=pltpu.CompilerParams(vmem_limit_bytes=VMEM_LIMIT),
    )(*operands)


def in_hbm(value):
    return pltpu.with_memory_space_constraint(value, pltpu.HBM)


def float_shape(*shape):
    return jax.ShapeDtypeStruct(shape, jnp.float32)


def swap_blocks(blocks):
    count = len(blocks)
    return [blocks[0]] + [
        lax.ppermute(block, "col", [(s, s ^ step) for s in range(count)])
        for step, block in list(zip(steps(count), blocks))[1:]
    ]


def on_device(substrate, activator):
    row_count, col_count = substrate.shape
    bands, count = lax.axis_size("outer") * lax.axis_size("core"), lax.axis_size("col")
    total_rows, total_cols = row_count * bands, col_count * count
    height = row_count // count
    radix = total_cols // LANES
    width = total_cols // (bands * count)
    assert row_count == LANES and total_rows == total_cols and count & (count - 1) == 0
    packed = count == 4 and height == SUBLANES * count and width * count == LANES
    matrices = basis_matrices(total_rows)
    forward = split_constant(matrices)
    backward = split_constant(np.swapaxes(matrices, 1, 2))

    block = float_shape(2, height, col_count)
    blocks = swap_blocks(
        call(
            cut_kernel,
            [block] * count,
            [HBM] * 2,
            (in_hbm(substrate), in_hbm(activator)),
            [pltpu.SemaphoreType.DMA((count, 2))],
        )
    )
    table, forward, backward = call(
        lambda *refs: tables_kernel(total_rows, total_cols, width, *refs),
        [float_shape(radix // 2, 2 * LANES, LANES)]
        + [jax.ShapeDtypeStruct(constant.shape, constant.dtype) for constant in (forward, backward)],
        [HBM, HBM],
        (in_hbm(forward), in_hbm(backward)),
        [pltpu.SemaphoreType.DMA((2,))],
    )
    spectra = call(
        lambda *refs: forward_kernel(packed, *refs),
        float_shape(bands * count, 3 * SUBLANES, LANES) if packed else float_shape(radix, 3 * height, LANES),
        [VMEM] * (count + 1),
        (*blocks, forward),
        [pltpu.VMEM((count, 2, height, col_count), jnp.float32)],
    )
    if packed:
        spectra = lax.all_to_all(spectra, AXES, 0, 0, tiled=True)
    else:
        spectra = spectra.reshape(radix, 3, height, LANES // width, width)
        spectra = jnp.transpose(spectra, (0, 3, 1, 2, 4)).reshape(bands * count, -1)
        spectra = lax.all_to_all(spectra, AXES, 0, 0, tiled=True)
        spectra = spectra.reshape(count, CORES, bands // CORES, 3, height, width)
        spectra = jnp.transpose(spectra, (3, 2, 1, 0, 4, 5))
        spectra = spectra.reshape(3, bands, row_count, width)
        rest = jnp.zeros((bands, row_count, HALF - 2 * width), jnp.float32)
        spectra = jnp.concatenate([spectra[0], spectra[1], rest, spectra[2], spectra[2], rest], axis=2)
    advanced = call(
        lambda *refs: advance_kernel(packed, count, *refs),
        float_shape(bands * count, 2 * SUBLANES, LANES) if packed else float_shape(bands, row_count, LANES),
        [VMEM] * 4,
        (spectra, table, forward, backward),
    )
    if packed:
        advanced = lax.all_to_all(advanced, AXES, 0, 0, tiled=True)
    else:
        advanced = advanced[:, :, : 2 * width].reshape(bands // CORES, CORES, count, height, 2, width)
        advanced = jnp.transpose(advanced, (2, 1, 0, 4, 3, 5)).reshape(bands * count, -1)
        advanced = lax.all_to_all(advanced, AXES, 0, 0, tiled=True)
        advanced = jnp.transpose(advanced.reshape(radix, LANES // width, 2, height, width), (0, 2, 3, 1, 4))
        advanced = advanced.reshape(radix, 2 * height, LANES)
    shift = FEED_RATE * math.expm1(-FEED_RATE * 0.5 * TIME_STEP) / -FEED_RATE
    blocks = swap_blocks(
        call(
            lambda *refs: inverse_kernel(packed, count, shift, *refs),
            [block] * count,
            [VMEM] * 2,
            (advanced, backward),
            [pltpu.VMEM((count, 2, height, col_count), jnp.float32)],
        )
    )
    return tuple(
        call(
            join_kernel,
            [float_shape(row_count, col_count)] * 2,
            [VMEM] * count,
            (*blocks,),
            [pltpu.SemaphoreType.DMA((count, 2))],
            HBM,
        )
    )


def solution(mesh):
    bands, count = mesh.shape["row"], mesh.shape["col"]
    split = Mesh(mesh.devices.reshape(bands // CORES, CORES, count), ("outer", "core", "col"))
    spec = P(("outer", "core"), "col")
    return jax.shard_map(on_device, mesh=split, in_specs=(spec, spec), out_specs=(spec, spec), check_vma=False)
```

```python
import math

import jax
import jax.numpy as jnp
import numpy as np
from jax import lax
from jax.experimental import pallas as pl
from jax.experimental.pallas import tpu as pltpu
from jax.sharding import Mesh
from jax.sharding import PartitionSpec as P

FEED_RATE = 0.037
KILL_RATE = 0.06
TIME_STEP = 8.0
SUBSTRATE_DIFFUSION = 4e-07
ACTIVATOR_DIFFUSION = 2e-07
LANES = 128
HALF = LANES // 2
CORES = 2
AXES = ("col", "core", "outer")
SUBLANES = 8
VMEM_LIMIT = 36 << 20
VMEM = pl.BlockSpec(memory_space=pltpu.VMEM)
HBM = pl.BlockSpec(memory_space=pltpu.HBM)


def basis_matrices(total):
    radix = total // LANES
    b = np.arange(LANES, dtype=np.int64)[:, None]
    k2 = np.arange(LANES, dtype=np.int64)[None, :]

    def angles(k1):
        return (b * (k1 + radix * k2) % total) * (2.0 * np.pi / total)

    matrices = np.zeros((radix // 2, 2 * LANES, 2 * LANES))
    for half, k1 in enumerate((0, radix // 2)):
        theta = angles(k1)
        part = slice(half * LANES, (half + 1) * LANES)
        matrices[0, part, part] = np.cos(theta) + np.sin(theta)
    for k1 in range(1, radix // 2):
        cosine, sine = np.cos(angles(k1)), np.sin(angles(k1))
        matrices[k1] = np.block([[cosine, -sine], [sine, cosine]])
    return matrices


def split_constant(matrices):
    high = matrices.astype(jnp.bfloat16)
    low = (matrices - high.astype(np.float64)).astype(jnp.bfloat16)
    return jnp.asarray(np.stack([high, low]))


def split_value(values):
    high = values.astype(jnp.bfloat16)
    low = (values - high.astype(jnp.float32)).astype(jnp.bfloat16)
    return high, low


def dot(left, right):
    return jnp.dot(left, right, preferred_element_type=jnp.float32)


def dot_pairs(left, right):
    height = left[0].shape[0]
    both = dot(jnp.concatenate(left, axis=0), right[0])
    return both[:height] + (both[height:] + dot(left[0], right[1]))


def turn(value, k, period, sign):
    real, imag = value
    if k == 0:
        return value
    if 4 * k == period:
        return (-sign * imag, sign * real) if imag is not None else (None, sign * real)
    cosine, sine = math.cos(2.0 * math.pi * k / period), sign * math.sin(2.0 * math.pi * k / period)
    if imag is None:
        return (real * cosine, real * sine)
    if 8 * k == period:
        return ((real - sign * imag) * cosine, (imag + sign * real) * cosine)
    return (real * cosine - imag * sine, real * sine + imag * cosine)


def plus(left, right):
    if left is None or right is None:
        return left if right is None else right
    return left + right


def minus(left, right):
    if right is None:
        return left
    return -right if left is None else left - right


def real_dft(values):
    n = len(values)
    if n == 1:
        return [(values[0], None)]
    even, odd = real_dft(values[0::2]), real_dft(values[1::2])
    out = [None] * (n // 2 + 1)
    for k in range(n // 4 + 1):
        turned = turn(odd[k], k, n, -1.0)
        if n // 2 - k != k:
            out[n // 2 - k] = (minus(even[k][0], turned[0]), minus(turned[1], even[k][1]))
        out[k] = (plus(even[k][0], turned[0]), plus(even[k][1], turned[1]))
    return out


def real_dft_transposed(spectrum):
    n = 2 * (len(spectrum) - 1)
    if n == 0:
        return [spectrum[0][0]]
    even, odd = [], []
    for k in range(n // 4 + 1):
        near, far = spectrum[k], spectrum[n // 2 - k]
        if k == 0:
            even.append((near[0] + far[0], None))
            odd.append((near[0] - far[0], None))
        elif 4 * k == n:
            even.append((near[0], None))
            odd.append((-near[1], None))
        else:
            even.append((near[0] + far[0], near[1] - far[1]))
            odd.append(turn((near[0] - far[0], near[1] + far[1]), k, n, 1.0))
    out = [None] * n
    out[0::2] = real_dft_transposed(even)
    out[1::2] = real_dft_transposed(odd)
    return out


def paired(spectrum, axis):
    half = len(spectrum) - 1
    rows = [(spectrum[0][0], spectrum[half][0])] + spectrum[1:half]
    return [jnp.concatenate(row, axis=axis) for row in rows]


def unpaired(products, axis):
    def halves(value):
        return lax.slice_in_dim(value, 0, LANES, axis=axis), lax.slice_in_dim(value, LANES, 2 * LANES, axis=axis)

    parts = [halves(value) for value in products]
    first, last = parts[0]
    return [(first, None)] + parts[1:] + [(last, None)]


def lane_chunk(shape, width):
    return lax.broadcasted_iota(jnp.int32, shape, len(shape) - 1) // width


def swap_chunks(pieces):
    pieces = list(pieces)
    count = len(pieces)
    width = LANES // count
    chunk = lane_chunk(pieces[0].shape, width)
    step = count // 2
    while step:
        stays = chunk & step == 0
        for first in range(count):
            if first & step:
                continue
            near, far = pieces[first], pieces[first + step]
            pieces[first] = jnp.where(stays, near, pltpu.roll(far, step * width, 1))
            pieces[first + step] = jnp.where(stays, pltpu.roll(near, LANES - step * width, 1), far)
        step //= 2
    return pieces


def sublane_rows(value, group):
    return value[group * SUBLANES : (group + 1) * SUBLANES]


def wave_squares(k1, k2, total):
    radix = total // LANES
    wave = k1 + radix * k2
    signed = jnp.where(2 * wave < total, wave, wave - total).astype(jnp.float32)
    angular = (2.0 * math.pi) * signed
    return angular * angular


def tables_kernel(total_rows, total_cols, width, *refs):
    *matrix_refs, table_ref, loaded_ref, loaded_t_ref, semaphores = refs
    copies = [
        pltpu.make_async_copy(source, target, semaphores.at[index])
        for index, (source, target) in enumerate(zip(matrix_refs, (loaded_ref, loaded_t_ref)))
    ]
    for copy in copies:
        copy.start()
    radix = total_rows // LANES
    chunks = LANES // width
    device = lax.axis_index(AXES)
    tile, place = device // chunks, device % chunks
    lane = lax.broadcasted_iota(jnp.int32, (1, LANES), 1)
    col_class = jnp.where(tile == 0, 0, jnp.where(tile == 1, total_cols // LANES // 2, tile // 2))
    col_squares = wave_squares(col_class, place * width + lane % width, total_cols)
    col_scale = jnp.where(tile < 2, 1.0 / total_cols, 2.0 / total_cols).astype(jnp.float32)
    first = lane % HALF < width
    diffusion = jnp.where(first, SUBSTRATE_DIFFUSION, ACTIVATOR_DIFFUSION).astype(jnp.float32)
    decay = jnp.where(first, FEED_RATE, FEED_RATE + KILL_RATE).astype(jnp.float32)
    sign = jnp.where(first, -1.0, 1.0).astype(jnp.float32)
    k2 = lax.broadcasted_iota(jnp.int32, (LANES, LANES), 0)
    for index in range(radix // 2):
        for half in range(2):
            k1 = half * (radix // 2) if index == 0 else index
            scale = col_scale * ((1.0 if index == 0 else 2.0) / total_rows)
            linear = -diffusion * (wave_squares(k1, k2, total_rows) + col_squares) - decay
            growth = jnp.exp(linear * (0.5 * TIME_STEP))
            rows = slice(half * LANES, (half + 1) * LANES)
            forcing = (growth - 1.0) / linear * sign
            table_ref[index, rows, :] = jnp.where(lane < HALF, growth, forcing) * scale
    for copy in copies:
        copy.wait()


def forward_kernel(packed, *refs):
    *block_refs, matrix_ref, out_ref, buffer_ref = refs
    count = len(block_refs)
    place = lax.axis_index("col")
    for step, block_ref in zip(steps(count), block_refs):
        buffer_ref[place ^ step] = block_ref[...]
    cols = buffer_ref.shape[-1]
    height = buffer_ref.shape[2]
    tiles = []
    for source in range(count):
        for tile in range(cols // LANES):
            part = slice(tile * LANES, (tile + 1) * LANES)
            substrate = buffer_ref[source, 0, :, part]
            activator = buffer_ref[source, 1, :, part]
            tiles.append(jnp.concatenate([substrate, activator, substrate * activator * activator], axis=0))
    operands = paired(real_dft(tiles), 1)
    for index, operand in enumerate(operands):
        product = dot_pairs(split_value(operand), (matrix_ref[0, index], matrix_ref[1, index]))
        for half in range(2):
            tile = 2 * index + half
            spectrum = product[:, half * LANES : (half + 1) * LANES]
            if not packed:
                out_ref[tile] = spectrum
                continue
            for field in range(3):
                part = spectrum[field * height : (field + 1) * height]
                for chunk, piece in enumerate(swap_chunks([sublane_rows(part, group) for group in range(count)])):
                    out_ref[tile * count + chunk, field * SUBLANES : (field + 1) * SUBLANES, :] = piece


def place_of(band, source, bands):
    return (source * CORES + band % CORES) * (bands // CORES) + band // CORES


def advance_kernel(packed, count, in_ref, table_ref, matrix_ref, matrix_t_ref, out_ref):
    if packed:
        radix = in_ref.shape[0] // count
        tiles = []
        for band in range(radix):
            rows = []
            for source in range(count):
                block = in_ref[place_of(band, source, radix)]
                rows += swap_chunks([sublane_rows(block, min(field, 2)) for field in range(count)])
            tiles.append(jnp.concatenate(rows, axis=0))
    else:
        radix = in_ref.shape[0]
        tiles = [in_ref[band] for band in range(radix)]
    operands = paired(real_dft(tiles), 0)
    low_half = lax.broadcasted_iota(jnp.int32, (2 * LANES, LANES), 1) < HALF
    scaled = []
    for index, operand in enumerate(operands):
        high, low = split_value(operand)
        both = dot(matrix_t_ref[0, index], jnp.concatenate([high, low], axis=1))
        spectrum = both[:, :LANES] + (both[:, LANES:] + dot(matrix_t_ref[1, index], high))
        scaled.append(table_ref[index] * spectrum)
    products = []
    for index, value in enumerate(scaled):
        advanced = value + pltpu.roll(value, HALF, 1)
        high = advanced.astype(jnp.bfloat16).astype(jnp.float32)
        both = dot(matrix_ref[0, index], jnp.where(low_half, high, advanced - high).astype(jnp.bfloat16))
        rest = dot(matrix_ref[1, index], high.astype(jnp.bfloat16))
        products.append(both + (pltpu.roll(both, HALF, 1) + rest))
    bands = real_dft_transposed(unpaired(products, 0))
    low_half = lane_chunk((SUBLANES, LANES), HALF) == 0
    even = lane_chunk((SUBLANES, LANES), HALF // 2) % 2 == 0
    for band, value in enumerate(bands):
        if not packed:
            out_ref[band] = value
            continue
        for target in range(count):
            part = value[target * LANES // count : (target + 1) * LANES // count]
            near = jnp.where(low_half, sublane_rows(part, 0), sublane_rows(part, 2))
            far = jnp.where(low_half, sublane_rows(part, 1), sublane_rows(part, 3))
            place = place_of(band, target, radix)
            out_ref[place, :SUBLANES, :] = jnp.where(even, near, pltpu.roll(far, HALF // 2, 1))
            out_ref[place, SUBLANES:, :] = jnp.where(even, pltpu.roll(near, LANES - HALF // 2, 1), far)


def inverse_kernel(packed, count, shift, in_ref, matrix_t_ref, *refs):
    place = lax.axis_index("col")
    *out_refs, buffer_ref = refs
    radix = 2 * matrix_t_ref.shape[1]
    _, height, cols = out_refs[0].shape
    tiles = []
    for tile in range(radix):
        if not packed:
            tiles.append(in_ref[tile])
            continue
        rows = []
        for field in range(2):
            rows += swap_chunks([sublane_rows(in_ref[tile * count + chunk], field) for chunk in range(count)])
        tiles.append(jnp.concatenate(rows, axis=0))
    products = []
    for index in range(radix // 2):
        operand = jnp.concatenate([tiles[2 * index], tiles[2 * index + 1]], axis=1)
        products.append(dot_pairs(split_value(operand), (matrix_t_ref[0, index], matrix_t_ref[1, index])))
    values = real_dft_transposed(unpaired(products, 1))
    per_target = cols // LANES
    for index, value in enumerate(values):
        target, tile = index // per_target, index % per_target
        part = slice(tile * LANES, (tile + 1) * LANES)
        buffer_ref[place ^ target, 0, :, part] = value[:height] + shift
        buffer_ref[place ^ target, 1, :, part] = value[height:]
    for step, out_ref in zip(steps(count), out_refs):
        out_ref[...] = buffer_ref[step]


def steps(count):
    return [0, count - 1] + list(range(1, count - 1))


def start_all(copies):
    for copy in copies:
        copy.start()
    for copy in copies:
        copy.wait()


def cut_kernel(*refs):
    *field_refs, semaphores = refs
    in_refs, out_refs = field_refs[:2], field_refs[2:]
    height = out_refs[0].shape[1]
    copies = []
    for index, (step, out_ref) in enumerate(zip(steps(len(out_refs)), out_refs)):
        rows = pl.ds((lax.axis_index("col") ^ step) * height, height)
        for field, in_ref in enumerate(in_refs):
            copies.append(pltpu.make_async_copy(in_ref.at[rows], out_ref.at[field], semaphores.at[index, field]))
    start_all(copies)


def join_kernel(*refs):
    *block_refs, first_ref, second_ref, buffer_ref, semaphores = refs
    height = block_refs[0].shape[1]
    for step, block_ref in zip(steps(len(block_refs)), block_refs):
        buffer_ref[:, pl.ds((lax.axis_index("col") ^ step) * height, height), :] = block_ref[...]
    start_all(
        [
            pltpu.make_async_copy(buffer_ref.at[field], out_ref, semaphores.at[field])
            for field, out_ref in enumerate((first_ref, second_ref))
        ]
    )


def call(kernel, out_shape, specs, operands, scratch=(), out_spec=VMEM):
    return pl.pallas_call(
        kernel,
        out_shape=out_shape,
        in_specs=specs,
        out_specs=jax.tree.map(lambda _: out_spec, out_shape),
        scratch_shapes=list(scratch),
        compiler_params=pltpu.CompilerParams(vmem_limit_bytes=VMEM_LIMIT),
    )(*operands)


def in_hbm(value):
    return pltpu.with_memory_space_constraint(value, pltpu.HBM)


def float_shape(*shape):
    return jax.ShapeDtypeStruct(shape, jnp.float32)


def swap_blocks(blocks):
    count = len(blocks)
    return [blocks[0]] + [
        lax.ppermute(block, "col", [(s, s ^ step) for s in range(count)])
        for step, block in list(zip(steps(count), blocks))[1:]
    ]


def on_device(substrate, activator):
    row_count, col_count = substrate.shape
    bands, count = lax.axis_size("outer") * lax.axis_size("core"), lax.axis_size("col")
    total_rows, total_cols = row_count * bands, col_count * count
    height = row_count // count
    radix = total_cols // LANES
    width = total_cols // (bands * count)
    assert row_count == LANES and total_rows == total_cols and count & (count - 1) == 0
    packed = count == 4 and height == SUBLANES * count and width * count == LANES
    matrices = basis_matrices(total_rows)
    forward = split_constant(matrices)
    backward = split_constant(np.swapaxes(matrices, 1, 2))

    block = float_shape(2, height, col_count)
    blocks = swap_blocks(
        call(
            cut_kernel,
            [block] * count,
            [HBM] * 2,
            (in_hbm(substrate), in_hbm(activator)),
            [pltpu.SemaphoreType.DMA((count, 2))],
        )
    )
    table, forward, backward = call(
        lambda *refs: tables_kernel(total_rows, total_cols, width, *refs),
        [float_shape(radix // 2, 2 * LANES, LANES)]
        + [jax.ShapeDtypeStruct(constant.shape, constant.dtype) for constant in (forward, backward)],
        [HBM, HBM],
        (in_hbm(forward), in_hbm(backward)),
        [pltpu.SemaphoreType.DMA((2,))],
    )
    spectra = call(
        lambda *refs: forward_kernel(packed, *refs),
        float_shape(bands * count, 3 * SUBLANES, LANES) if packed else float_shape(radix, 3 * height, LANES),
        [VMEM] * (count + 1),
        (*blocks, forward),
        [pltpu.VMEM((count, 2, height, col_count), jnp.float32)],
    )
    if packed:
        spectra = lax.all_to_all(spectra, AXES, 0, 0, tiled=True)
    else:
        spectra = spectra.reshape(radix, 3, height, LANES // width, width)
        spectra = jnp.transpose(spectra, (0, 3, 1, 2, 4)).reshape(bands * count, -1)
        spectra = lax.all_to_all(spectra, AXES, 0, 0, tiled=True)
        spectra = spectra.reshape(count, CORES, bands // CORES, 3, height, width)
        spectra = jnp.transpose(spectra, (3, 2, 1, 0, 4, 5))
        spectra = spectra.reshape(3, bands, row_count, width)
        rest = jnp.zeros((bands, row_count, HALF - 2 * width), jnp.float32)
        spectra = jnp.concatenate([spectra[0], spectra[1], rest, spectra[2], spectra[2], rest], axis=2)
    advanced = call(
        lambda *refs: advance_kernel(packed, count, *refs),
        float_shape(bands * count, 2 * SUBLANES, LANES) if packed else float_shape(bands, row_count, LANES),
        [VMEM] * 4,
        (spectra, table, forward, backward),
    )
    if packed:
        advanced = lax.all_to_all(advanced, AXES, 0, 0, tiled=True)
    else:
        advanced = advanced[:, :, : 2 * width].reshape(bands // CORES, CORES, count, height, 2, width)
        advanced = jnp.transpose(advanced, (2, 1, 0, 4, 3, 5)).reshape(bands * count, -1)
        advanced = lax.all_to_all(advanced, AXES, 0, 0, tiled=True)
        advanced = jnp.transpose(advanced.reshape(radix, LANES // width, 2, height, width), (0, 2, 3, 1, 4))
        advanced = advanced.reshape(radix, 2 * height, LANES)
    shift = FEED_RATE * math.expm1(-FEED_RATE * 0.5 * TIME_STEP) / -FEED_RATE
    blocks = swap_blocks(
        call(
            lambda *refs: inverse_kernel(packed, count, shift, *refs),
            [block] * count,
            [VMEM] * 2,
            (advanced, backward),
            [pltpu.VMEM((count, 2, height, col_count), jnp.float32)],
        )
    )
    return tuple(
        call(
            join_kernel,
            [float_shape(row_count, col_count)] * 2,
            [VMEM] * count,
            (*blocks,),
            [pltpu.VMEM((2, row_count, col_count), jnp.float32), pltpu.SemaphoreType.DMA((2,))],
            HBM,
        )
    )


def solution(mesh):
    bands, count = mesh.shape["row"], mesh.shape["col"]
    split = Mesh(mesh.devices.reshape(bands // CORES, CORES, count), ("outer", "core", "col"))
    spec = P(("outer", "core"), "col")
    return jax.shard_map(on_device, mesh=split, in_specs=(spec, spec), out_specs=(spec, spec), check_vma=False)
```

```python
import math

import jax
import jax.numpy as jnp
import numpy as np
from jax import lax
from jax.experimental import pallas as pl
from jax.experimental.pallas import tpu as pltpu
from jax.sharding import Mesh
from jax.sharding import PartitionSpec as P

FEED_RATE = 0.037
KILL_RATE = 0.06
TIME_STEP = 8.0
SUBSTRATE_DIFFUSION = 4e-07
ACTIVATOR_DIFFUSION = 2e-07
LANES = 128
HALF = LANES // 2
CORES = 2
AXES = ("col", "core", "outer")
SUBLANES = 8
VMEM_LIMIT = 36 << 20
VMEM = pl.BlockSpec(memory_space=pltpu.VMEM)
HBM = pl.BlockSpec(memory_space=pltpu.HBM)


def basis_matrices(total):
    radix = total // LANES
    b = np.arange(LANES, dtype=np.int64)[:, None]
    k2 = np.arange(LANES, dtype=np.int64)[None, :]

    def angles(k1):
        return (b * (k1 + radix * k2) % total) * (2.0 * np.pi / total)

    matrices = np.zeros((radix // 2, 2 * LANES, 2 * LANES))
    for half, k1 in enumerate((0, radix // 2)):
        theta = angles(k1)
        part = slice(half * LANES, (half + 1) * LANES)
        matrices[0, part, part] = np.cos(theta) + np.sin(theta)
    for k1 in range(1, radix // 2):
        cosine, sine = np.cos(angles(k1)), np.sin(angles(k1))
        matrices[k1] = np.block([[cosine, -sine], [sine, cosine]])
    return matrices


def split_constant(matrices):
    high = matrices.astype(jnp.bfloat16)
    low = (matrices - high.astype(np.float64)).astype(jnp.bfloat16)
    return jnp.asarray(np.stack([high, low]))


def split_value(values):
    high = values.astype(jnp.bfloat16)
    low = (values - high.astype(jnp.float32)).astype(jnp.bfloat16)
    return high, low


def dot(left, right):
    return jnp.dot(left, right, preferred_element_type=jnp.float32)


def dot_pairs(left, right):
    height = left[0].shape[0]
    both = dot(jnp.concatenate(left, axis=0), right[0])
    return both[:height] + (both[height:] + dot(left[0], right[1]))


def turn(value, k, period, sign):
    real, imag = value
    if k == 0:
        return value
    if 4 * k == period:
        return (-sign * imag, sign * real) if imag is not None else (None, sign * real)
    cosine, sine = math.cos(2.0 * math.pi * k / period), sign * math.sin(2.0 * math.pi * k / period)
    if imag is None:
        return (real * cosine, real * sine)
    if 8 * k == period:
        return ((real - sign * imag) * cosine, (imag + sign * real) * cosine)
    return (real * cosine - imag * sine, real * sine + imag * cosine)


def plus(left, right):
    if left is None or right is None:
        return left if right is None else right
    return left + right


def minus(left, right):
    if right is None:
        return left
    return -right if left is None else left - right


def real_dft(values):
    n = len(values)
    if n == 1:
        return [(values[0], None)]
    even, odd = real_dft(values[0::2]), real_dft(values[1::2])
    out = [None] * (n // 2 + 1)
    for k in range(n // 4 + 1):
        turned = turn(odd[k], k, n, -1.0)
        if n // 2 - k != k:
            out[n // 2 - k] = (minus(even[k][0], turned[0]), minus(turned[1], even[k][1]))
        out[k] = (plus(even[k][0], turned[0]), plus(even[k][1], turned[1]))
    return out


def real_dft_transposed(spectrum):
    n = 2 * (len(spectrum) - 1)
    if n == 0:
        return [spectrum[0][0]]
    even, odd = [], []
    for k in range(n // 4 + 1):
        near, far = spectrum[k], spectrum[n // 2 - k]
        if k == 0:
            even.append((near[0] + far[0], None))
            odd.append((near[0] - far[0], None))
        elif 4 * k == n:
            even.append((near[0], None))
            odd.append((-near[1], None))
        else:
            even.append((near[0] + far[0], near[1] - far[1]))
            odd.append(turn((near[0] - far[0], near[1] + far[1]), k, n, 1.0))
    out = [None] * n
    out[0::2] = real_dft_transposed(even)
    out[1::2] = real_dft_transposed(odd)
    return out


def paired(spectrum, axis):
    half = len(spectrum) - 1
    rows = [(spectrum[0][0], spectrum[half][0])] + spectrum[1:half]
    return [jnp.concatenate(row, axis=axis) for row in rows]


def unpaired(products, axis):
    def halves(value):
        return lax.slice_in_dim(value, 0, LANES, axis=axis), lax.slice_in_dim(value, LANES, 2 * LANES, axis=axis)

    parts = [halves(value) for value in products]
    first, last = parts[0]
    return [(first, None)] + parts[1:] + [(last, None)]


def lane_chunk(shape, width):
    return lax.broadcasted_iota(jnp.int32, shape, len(shape) - 1) // width


def swap_chunks(pieces):
    pieces = list(pieces)
    count = len(pieces)
    width = LANES // count
    chunk = lane_chunk(pieces[0].shape, width)
    step = count // 2
    while step:
        stays = chunk & step == 0
        for first in range(count):
            if first & step:
                continue
            near, far = pieces[first], pieces[first + step]
            pieces[first] = jnp.where(stays, near, pltpu.roll(far, step * width, 1))
            pieces[first + step] = jnp.where(stays, pltpu.roll(near, LANES - step * width, 1), far)
        step //= 2
    return pieces


def sublane_rows(value, group):
    return value[group * SUBLANES : (group + 1) * SUBLANES]


def wave_squares(k1, k2, total):
    radix = total // LANES
    wave = k1 + radix * k2
    signed = jnp.where(2 * wave < total, wave, wave - total).astype(jnp.float32)
    angular = (2.0 * math.pi) * signed
    return angular * angular


def tables_kernel(total_rows, total_cols, width, *refs):
    *matrix_refs, table_ref, loaded_ref, loaded_t_ref, semaphores = refs
    copies = [
        pltpu.make_async_copy(source, target, semaphores.at[index])
        for index, (source, target) in enumerate(zip(matrix_refs, (loaded_ref, loaded_t_ref)))
    ]
    for copy in copies:
        copy.start()
    radix = total_rows // LANES
    chunks = LANES // width
    device = lax.axis_index(AXES)
    tile, place = device // chunks, device % chunks
    lane = lax.broadcasted_iota(jnp.int32, (1, LANES), 1)
    col_class = jnp.where(tile == 0, 0, jnp.where(tile == 1, total_cols // LANES // 2, tile // 2))
    col_squares = wave_squares(col_class, place * width + lane % width, total_cols)
    col_scale = jnp.where(tile < 2, 1.0 / total_cols, 2.0 / total_cols).astype(jnp.float32)
    first = lane % HALF < width
    diffusion = jnp.where(first, SUBSTRATE_DIFFUSION, ACTIVATOR_DIFFUSION).astype(jnp.float32)
    decay = jnp.where(first, FEED_RATE, FEED_RATE + KILL_RATE).astype(jnp.float32)
    sign = jnp.where(first, -1.0, 1.0).astype(jnp.float32)
    k2 = lax.broadcasted_iota(jnp.int32, (LANES, LANES), 0)
    for index in range(radix // 2):
        for half in range(2):
            k1 = half * (radix // 2) if index == 0 else index
            scale = col_scale * ((1.0 if index == 0 else 2.0) / total_rows)
            linear = -diffusion * (wave_squares(k1, k2, total_rows) + col_squares) - decay
            growth = jnp.exp(linear * (0.5 * TIME_STEP))
            rows = slice(half * LANES, (half + 1) * LANES)
            forcing = (growth - 1.0) / linear * sign
            table_ref[index, rows, :] = jnp.where(lane < HALF, growth, forcing) * scale
    for copy in copies:
        copy.wait()


def forward_kernel(packed, *refs):
    *block_refs, matrix_ref, out_ref, buffer_ref = refs
    count = len(block_refs)
    place = lax.axis_index("col")
    for step, block_ref in zip(steps(count), block_refs):
        buffer_ref[place ^ step] = block_ref[...]
    cols = buffer_ref.shape[-1]
    height = buffer_ref.shape[2]
    tiles = []
    for source in range(count):
        for tile in range(cols // LANES):
            part = slice(tile * LANES, (tile + 1) * LANES)
            substrate = buffer_ref[source, 0, :, part]
            activator = buffer_ref[source, 1, :, part]
            tiles.append(jnp.concatenate([substrate, activator, substrate * activator * activator], axis=0))
    operands = paired(real_dft(tiles), 1)
    for index, operand in enumerate(operands):
        product = dot_pairs(split_value(operand), (matrix_ref[0, index], matrix_ref[1, index]))
        for half in range(2):
            tile = 2 * index + half
            spectrum = product[:, half * LANES : (half + 1) * LANES]
            if not packed:
                out_ref[tile] = spectrum
                continue
            for field in range(3):
                part = spectrum[field * height : (field + 1) * height]
                for chunk, piece in enumerate(swap_chunks([sublane_rows(part, group) for group in range(count)])):
                    out_ref[tile * count + chunk, field * SUBLANES : (field + 1) * SUBLANES, :] = piece


def place_of(band, source, bands):
    return (source * CORES + band % CORES) * (bands // CORES) + band // CORES


def advance_kernel(packed, count, in_ref, table_ref, matrix_ref, matrix_t_ref, out_ref):
    if packed:
        radix = in_ref.shape[0] // count
        tiles = []
        for band in range(radix):
            rows = []
            for source in range(count):
                block = in_ref[place_of(band, source, radix)]
                rows += swap_chunks([sublane_rows(block, min(field, 2)) for field in range(count)])
            tiles.append(jnp.concatenate(rows, axis=0))
    else:
        radix = in_ref.shape[0]
        tiles = [in_ref[band] for band in range(radix)]
    operands = paired(real_dft(tiles), 0)
    low_half = lax.broadcasted_iota(jnp.int32, (2 * LANES, LANES), 1) < HALF
    scaled = []
    for index, operand in enumerate(operands):
        high, low = split_value(operand)
        both = dot(matrix_t_ref[0, index], jnp.concatenate([high, low], axis=1))
        spectrum = both[:, :LANES] + (both[:, LANES:] + dot(matrix_t_ref[1, index], high))
        scaled.append(table_ref[index] * spectrum)
    products = []
    for index, value in enumerate(scaled):
        advanced = value + pltpu.roll(value, HALF, 1)
        high = advanced.astype(jnp.bfloat16).astype(jnp.float32)
        both = dot(matrix_ref[0, index], jnp.where(low_half, high, advanced - high).astype(jnp.bfloat16))
        rest = dot(matrix_ref[1, index], high.astype(jnp.bfloat16))
        products.append(both + (pltpu.roll(both, HALF, 1) + rest))
    bands = real_dft_transposed(unpaired(products, 0))
    low_half = lane_chunk((SUBLANES, LANES), HALF) == 0
    even = lane_chunk((SUBLANES, LANES), HALF // 2) % 2 == 0
    for band, value in enumerate(bands):
        if not packed:
            out_ref[band] = value
            continue
        for target in range(count):
            part = value[target * LANES // count : (target + 1) * LANES // count]
            near = jnp.where(low_half, sublane_rows(part, 0), sublane_rows(part, 2))
            far = jnp.where(low_half, sublane_rows(part, 1), sublane_rows(part, 3))
            place = place_of(band, target, radix)
            out_ref[place, :SUBLANES, :] = jnp.where(even, near, pltpu.roll(far, HALF // 2, 1))
            out_ref[place, SUBLANES:, :] = jnp.where(even, pltpu.roll(near, LANES - HALF // 2, 1), far)


def inverse_kernel(packed, count, shift, in_ref, matrix_t_ref, *refs):
    place = lax.axis_index("col")
    *out_refs, buffer_ref = refs
    radix = 2 * matrix_t_ref.shape[1]
    _, height, cols = out_refs[0].shape
    tiles = []
    for tile in range(radix):
        if not packed:
            tiles.append(in_ref[tile])
            continue
        rows = []
        for field in range(2):
            rows += swap_chunks([sublane_rows(in_ref[tile * count + chunk], field) for chunk in range(count)])
        tiles.append(jnp.concatenate(rows, axis=0))
    products = []
    for index in range(radix // 2):
        operand = jnp.concatenate([tiles[2 * index], tiles[2 * index + 1]], axis=1)
        products.append(dot_pairs(split_value(operand), (matrix_t_ref[0, index], matrix_t_ref[1, index])))
    values = real_dft_transposed(unpaired(products, 1))
    per_target = cols // LANES
    for index, value in enumerate(values):
        target, tile = index // per_target, index % per_target
        part = slice(tile * LANES, (tile + 1) * LANES)
        buffer_ref[place ^ target, 0, :, part] = value[:height] + shift
        buffer_ref[place ^ target, 1, :, part] = value[height:]
    for step, out_ref in zip(steps(count), out_refs):
        out_ref[...] = buffer_ref[step]


def steps(count):
    return [0] + list(range(count - 1, 0, -1))


def start_all(copies):
    for copy in copies:
        copy.start()
    for copy in copies:
        copy.wait()


def cut_kernel(*refs):
    *field_refs, semaphores = refs
    in_refs, out_refs = field_refs[:2], field_refs[2:]
    height = out_refs[0].shape[1]
    copies = []
    for index, (step, out_ref) in enumerate(zip(steps(len(out_refs)), out_refs)):
        rows = pl.ds((lax.axis_index("col") ^ step) * height, height)
        for field, in_ref in enumerate(in_refs):
            copies.append(pltpu.make_async_copy(in_ref.at[rows], out_ref.at[field], semaphores.at[index, field]))
    start_all(copies)


def join_kernel(*refs):
    *block_refs, first_ref, second_ref, semaphores = refs
    height = block_refs[0].shape[1]
    copies = []
    for index, (step, block_ref) in enumerate(zip(steps(len(block_refs)), block_refs)):
        rows = pl.ds((lax.axis_index("col") ^ step) * height, height)
        for field, out_ref in enumerate((first_ref, second_ref)):
            copies.append(pltpu.make_async_copy(block_ref.at[field], out_ref.at[rows], semaphores.at[index, field]))
    start_all(copies)


def call(kernel, out_shape, specs, operands, scratch=(), out_spec=VMEM):
    return pl.pallas_call(
        kernel,
        out_shape=out_shape,
        in_specs=specs,
        out_specs=jax.tree.map(lambda _: out_spec, out_shape),
        scratch_shapes=list(scratch),
        compiler_params=pltpu.CompilerParams(vmem_limit_bytes=VMEM_LIMIT),
    )(*operands)


def in_hbm(value):
    return pltpu.with_memory_space_constraint(value, pltpu.HBM)


def float_shape(*shape):
    return jax.ShapeDtypeStruct(shape, jnp.float32)


def swap_blocks(blocks):
    count = len(blocks)
    return [blocks[0]] + [
        lax.ppermute(block, "col", [(s, s ^ step) for s in range(count)])
        for step, block in list(zip(steps(count), blocks))[1:]
    ]


def on_device(substrate, activator):
    row_count, col_count = substrate.shape
    bands, count = lax.axis_size("outer") * lax.axis_size("core"), lax.axis_size("col")
    total_rows, total_cols = row_count * bands, col_count * count
    height = row_count // count
    radix = total_cols // LANES
    width = total_cols // (bands * count)
    assert row_count == LANES and total_rows == total_cols and count & (count - 1) == 0
    packed = count == 4 and height == SUBLANES * count and width * count == LANES
    matrices = basis_matrices(total_rows)
    forward = split_constant(matrices)
    backward = split_constant(np.swapaxes(matrices, 1, 2))

    block = float_shape(2, height, col_count)
    blocks = swap_blocks(
        call(
            cut_kernel,
            [block] * count,
            [HBM] * 2,
            (in_hbm(substrate), in_hbm(activator)),
            [pltpu.SemaphoreType.DMA((count, 2))],
        )
    )
    table, forward, backward = call(
        lambda *refs: tables_kernel(total_rows, total_cols, width, *refs),
        [float_shape(radix // 2, 2 * LANES, LANES)]
        + [jax.ShapeDtypeStruct(constant.shape, constant.dtype) for constant in (forward, backward)],
        [HBM, HBM],
        (in_hbm(forward), in_hbm(backward)),
        [pltpu.SemaphoreType.DMA((2,))],
    )
    spectra = call(
        lambda *refs: forward_kernel(packed, *refs),
        float_shape(bands * count, 3 * SUBLANES, LANES) if packed else float_shape(radix, 3 * height, LANES),
        [VMEM] * (count + 1),
        (*blocks, forward),
        [pltpu.VMEM((count, 2, height, col_count), jnp.float32)],
    )
    if packed:
        spectra = lax.all_to_all(spectra, AXES, 0, 0, tiled=True)
    else:
        spectra = spectra.reshape(radix, 3, height, LANES // width, width)
        spectra = jnp.transpose(spectra, (0, 3, 1, 2, 4)).reshape(bands * count, -1)
        spectra = lax.all_to_all(spectra, AXES, 0, 0, tiled=True)
        spectra = spectra.reshape(count, CORES, bands // CORES, 3, height, width)
        spectra = jnp.transpose(spectra, (3, 2, 1, 0, 4, 5))
        spectra = spectra.reshape(3, bands, row_count, width)
        rest = jnp.zeros((bands, row_count, HALF - 2 * width), jnp.float32)
        spectra = jnp.concatenate([spectra[0], spectra[1], rest, spectra[2], spectra[2], rest], axis=2)
    advanced = call(
        lambda *refs: advance_kernel(packed, count, *refs),
        float_shape(bands * count, 2 * SUBLANES, LANES) if packed else float_shape(bands, row_count, LANES),
        [VMEM] * 4,
        (spectra, table, forward, backward),
    )
    if packed:
        advanced = lax.all_to_all(advanced, AXES, 0, 0, tiled=True)
    else:
        advanced = advanced[:, :, : 2 * width].reshape(bands // CORES, CORES, count, height, 2, width)
        advanced = jnp.transpose(advanced, (2, 1, 0, 4, 3, 5)).reshape(bands * count, -1)
        advanced = lax.all_to_all(advanced, AXES, 0, 0, tiled=True)
        advanced = jnp.transpose(advanced.reshape(radix, LANES // width, 2, height, width), (0, 2, 3, 1, 4))
        advanced = advanced.reshape(radix, 2 * height, LANES)
    shift = FEED_RATE * math.expm1(-FEED_RATE * 0.5 * TIME_STEP) / -FEED_RATE
    blocks = swap_blocks(
        call(
            lambda *refs: inverse_kernel(packed, count, shift, *refs),
            [block] * count,
            [VMEM] * 2,
            (advanced, backward),
            [pltpu.VMEM((count, 2, height, col_count), jnp.float32)],
        )
    )
    return tuple(
        call(
            join_kernel,
            [float_shape(row_count, col_count)] * 2,
            [VMEM] * count,
            (*blocks,),
            [pltpu.SemaphoreType.DMA((count, 2))],
            HBM,
        )
    )


def solution(mesh):
    bands, count = mesh.shape["row"], mesh.shape["col"]
    split = Mesh(mesh.devices.reshape(bands // CORES, CORES, count), ("outer", "core", "col"))
    spec = P(("outer", "core"), "col")
    return jax.shard_map(on_device, mesh=split, in_specs=(spec, spec), out_specs=(spec, spec), check_vma=False)
```
